256 devices in a mesh: row: 32 (over x, z_lo, core), col: 8 (over z_hi, y).
Axes of the slice: x: 4, y: 4, z: 8 (z_hi: 2, z_lo: 4; z = z_hi * 4 + z_lo), core: 2. Of those that a mesh axis runs over, the one named last changes fastest.
Arguments:
- embed_first: bfloat16 [1536, 16384], P('col', 'row'), may hold values from -6 to 6
- embed_second: bfloat16 [1536, 16384], P('row', 'col'), may hold values from -6 to 6
- corr_grad: float32 [16384, 16384], P('row', 'col'), may hold values from -0.046875 to 0.046875
Outputs:
- grad_first: bfloat16 [1536, 16384], P('col', 'row')
- grad_second: bfloat16 [1536, 16384], P('row', 'col')
The draws below stay inside these ranges and needn't reach their ends.
All inputs are finite; a program needn't handle non-finite values.
Results may differ from the reference program's by a relative error of at most 0.0065.
Values may be sent and summed in bfloat16 or wider, within the bound.
A program may use at most 128 MiB of HBM per device.

```python
import jax
import jax.numpy as jnp
from jax import lax

F = 16384
BATCH = 1536


def levels(key, extent, cuts, low, high):
    def one(axis_at, shards_of):
        draws = jax.random.uniform(jax.random.fold_in(jax.random.fold_in(key, 6), axis_at), (shards_of,), jnp.float32, low / len(cuts), high / len(cuts))
        return jnp.repeat(jnp.exp(draws), extent[axis_at] // shards_of).reshape((-1,) + (1,) * (len(extent) - axis_at - 1))

    loudness = one(*cuts[0])
    for cut in cuts[1:]:
        loudness = loudness * one(*cut)
    return loudness


def noise(rng, shape, spread, limit, split=(), kind=jnp.bfloat16):
    gain = levels(rng, shape, split, -0.22, 0.18) if split else 1.0
    drawn = jax.random.normal(rng, shape, jnp.float32) * spread * gain
    return jnp.minimum(jnp.maximum(drawn, -limit), limit).astype(kind)


def setup_inputs(seed: int = 0) -> dict:
    splits = jax.random.split(jax.random.key(seed), 4)
    embed_first = noise(splits[0], (BATCH, F), 1.0, 6.0, ((0, 8), (1, 32)))
    embed_second = noise(splits[1], (BATCH, F), 1.0, 6.0, ((0, 32), (1, 8)))
    corr_grad = noise(splits[2], (F, F), F ** -0.5, 0.046875, ((0, 32), (1, 8)), jnp.float32)
    return {"embed_first": embed_first, "embed_second": embed_second, "corr_grad": corr_grad}


def reference(embed_first, embed_second, corr_grad):
    low_grad = corr_grad.astype(jnp.bfloat16)
    grad_first = lax.dot_general(embed_second, low_grad, (((1,), (1,)), ((), ())), preferred_element_type=jnp.float32)
    grad_second = jnp.dot(embed_first, low_grad, preferred_element_type=jnp.float32)
    return grad_first.astype(jnp.bfloat16), grad_second.astype(jnp.bfloat16)
```

```python
import jax
import jax.numpy as jnp
from jax import lax
from jax.experimental import pallas as pl
from jax.experimental.pallas import tpu as pltpu
from jax.sharding import PartitionSpec as P

BF = jnp.bfloat16
F32 = jnp.float32
MESH = pl.DeviceIdType.MESH


def kernel(e1_hbm, e2_hbm, g_hbm, gf_ref, gs_ref,
           e1s, E1, E2, gst, G, PS, PF, XA, XB, YA, YB, ZO, ZI, SZ, TZ, ZH, FS, FX,
           lsem, gsem, cs, cr, es, er, zs, zr, ys, yr, xs, xr, ps, pr, fs, fr, ss, sr):
    row = lax.axis_index("row")
    col = lax.axis_index("col")
    x, p, c = row // 8, (row // 2) % 4, row % 2
    zh, y = col // 4, col % 4
    s = 1 - 2 * (p // 2)
    mid = ((p + 1) // 2) % 2
    first = p // 2

    def dev(x_=x, p_=p, c_=c, zh_=zh, y_=y):
        return ((x_ * 4 + p_) * 2 + c_, zh_ * 4 + y_)

    xp, xm, xo = (x + 1) % 4, (x + 3) % 4, (x + 2) % 4
    yp, ym, yo = (y + 1) % 4, (y + 3) % 4, (y + 2) % 4
    d_core = dev(c_=1 - c)
    d_xp, d_xm = dev(x_=xp), dev(x_=xm)
    d_yp, d_ym = dev(y_=yp), dev(y_=ym)
    d_zh = dev(zh_=1 - zh)
    d_in = dev(p_=p + s)
    d_out = dev(p_=(p - s + 4) % 4)

    pending, block_sends = [], []

    def rc(src, dst, ssem, rsem, d):
        return pltpu.make_async_remote_copy(src, dst, ssem, rsem, device_id=d, device_id_type=MESH)

    def go(src, dst, ssem, rsem, d):
        cp = rc(src, dst, ssem, rsem, d)
        cp.start()
        pending.append(cp)

    def go_if(when, src, dst, sems, i, rsem, d):
        rc(src, dst, sems.at[i], rsem, d).start()
        block_sends.append((when, sems, i))

    def got(dst, rsem):
        rc(dst, dst, rsem, rsem, d_core).wait_recv()

    o = [p + s * (mid * m + (1 - mid) * e) for m, e in ((0, 0), (-1, 1), (1, 2), (2, 3))]
    t = [p + s * (mid * m + (1 - mid) * e) for m, e in ((2, 3), (1, 2), (-1, 1), (0, 0))]

    l2 = [pltpu.make_async_copy(e2_hbm.at[:, pl.ds(h * 1024, 1024)], E2.at[p, x, h], lsem.at[h]) for h in range(2)]
    l1 = pltpu.make_async_copy(e1_hbm, e1s, lsem.at[2])
    l1own = pltpu.make_async_copy(e1_hbm.at[:, c], E1.at[col, c], lsem.at[3])
    for cp in l2:
        cp.start()
    l1.start()
    l1own.start()
    lg = [pltpu.make_async_copy(g_hbm.at[pl.ds(i * 128, 128)], gst.at[i], gsem.at[i]) for i in range(4)]
    for cp in lg:
        cp.start()

    barrier = pltpu.get_barrier_semaphore()
    for d in (d_core, d_xp, d_xm, d_yp, d_ym, d_zh, d_in):
        pl.semaphore_signal(barrier, 1, device_id=d, device_id_type=MESH)

    @pl.when(mid == 1)
    def _():
        pl.semaphore_signal(barrier, 1, device_id=d_out, device_id_type=MESH)

    pl.semaphore_wait(barrier, 7 + mid)

    for cp in l2:
        cp.wait()

    @pl.when(mid == 1)
    def _():
        go_if(1, E2.at[p, x], E2.at[p, x], zs, 0, zr.at[0], d_in)
        go_if(1, E2.at[p, x], E2.at[p, x], zs, 1, zr.at[0], d_out)

    @pl.when(mid == 0)
    def _():
        go_if(0, E2.at[p, x], E2.at[p, x], zs, 0, zr.at[3], d_in)

    def x_full(k):
        go(E2.at[o[k], x], E2.at[o[k], x], xs.at[k, 0], xr.at[k, 0], d_xp)
        go(E2.at[o[k], x], E2.at[o[k], x], xs.at[k, 1], xr.at[k, 1], d_xm)

    def x_half(k):
        got(E2.at[o[k], xm], xr.at[k, 0])
        go(E2.at[o[k], xm, 0], E2.at[o[k], xm, 0], xs.at[k, 2], xr.at[k, 2], d_xp)
        got(E2.at[o[k], xp], xr.at[k, 1])
        go(E2.at[o[k], xp, 1], E2.at[o[k], xp, 1], xs.at[k, 3], xr.at[k, 3], d_xm)

    def x_end(k):
        got(E2.at[o[k], xo, 0], xr.at[k, 2])
        got(E2.at[o[k], xo, 1], xr.at[k, 3])

    zslot = [None] + [mid * m + (1 - mid) * e for m, e in ((3, 0), (0, 1), (1, 2))]

    def z_step(k):
        got(E2.at[o[k], x], zr.at[zslot[k]])
        x_full(k)

        @pl.when(mid == 1)
        def _():
            d = d_in if k == 1 else d_out
            slot = 1 if k < 3 else 2
            go_if(1, E2.at[o[k], x], E2.at[o[k], x], zs, k + 1, zr.at[slot], d)

    x_full(0)

    l1.wait()
    go(e1s.at[:, 1 - c], E1.at[col, c], cs.at[0], cr.at[0], d_core)
    l1own.wait()
    got(E1.at[col, 1 - c], cr.at[0])

    def y_full(i, q):
        go(E1.at[q * 4 + y], E1.at[q * 4 + y], ys.at[i, 0], yr.at[i, 0], d_yp)
        go(E1.at[q * 4 + y], E1.at[q * 4 + y], ys.at[i, 1], yr.at[i, 1], d_ym)

    def y_half(i, q):
        got(E1.at[q * 4 + ym], yr.at[i, 0])
        go(E1.at[q * 4 + ym, 0], E1.at[q * 4 + ym, 0], ys.at[i, 2], yr.at[i, 2], d_yp)
        got(E1.at[q * 4 + yp], yr.at[i, 1])
        go(E1.at[q * 4 + yp, 1], E1.at[q * 4 + yp, 1], ys.at[i, 3], yr.at[i, 3], d_ym)

    def y_end(i, q):
        got(E1.at[q * 4 + yo, 0], yr.at[i, 2])
        got(E1.at[q * 4 + yo, 1], yr.at[i, 3])

    y_full(0, zh)
    go(E1.at[col], E1.at[col], es.at[0], er.at[0], d_zh)

    for i in range(4):
        lg[i].wait()
        G[c, pl.ds(i * 128, 128), :] = gst[i].astype(BF)
        go(G.at[c, pl.ds(i * 128, 128)], G.at[c, pl.ds(i * 128, 128)], cs.at[1 + i], cr.at[1 + i], d_core)

    def gf_task(a):
        def body(j, carry):
            h, i = j // 2, j % 2
            acc = None
            for hj in range(2):
                lhs = E2[2 * a + i, :, hj].reshape(192, 1024)
                r = lax.dot_general(lhs, G[h, :, pl.ds(hj * 1024, 1024)], (((1,), (1,)), ((), ())),
                                    preferred_element_type=F32)
                acc = r if acc is None else acc + r
            acc = acc.astype(BF).reshape(4, 48, 512)
            for k in range(4):
                PF[2 * k + a, h, i] = acc[k]
            return carry
        lax.fori_loop(0, 4, body, 0)

    def gs_task(xx):
        def body(n, carry):
            acc = None
            for h in range(2):
                lhs = E1[pl.ds(2 * xx, 2), h].reshape(192, 512)
                r = jnp.dot(lhs, G[h, :, pl.ds(pl.multiple_of(n * 512, 512), 512)], preferred_element_type=F32)
                acc = r if acc is None else acc + r
            PS[xx, :, n // 2, :, pl.ds(pl.multiple_of((n % 2) * 512, 512), 512)] = acc.astype(BF).reshape(4, 48, 512)
            return carry
        lax.fori_loop(0, 4, body, 0)

    z_step(1)
    x_half(0)
    y_half(0, zh)
    z_step(2)
    x_half(1)
    for i in range(4):
        got(G.at[1 - c, pl.ds(i * 128, 128)], cr.at[1 + i])
    z_step(3)
    got(E1.at[(1 - zh) * 4 + y], er.at[0])
    y_full(1, 1 - zh)
    x_end(0)
    x_end(1)
    gf_task(first)
    x_half(2)
    y_half(1, 1 - zh)
    y_end(0, zh)
    y_end(1, 1 - zh)
    gs_task(xo)
    x_half(3)

    def xa(k):
        go(PS.at[xo, t[k], 0], XA.at[k, 0], ps.at[k, 0], pr.at[k, 0], d_xp)
        go(PS.at[xo, t[k], 1], XA.at[k, 1], ps.at[k, 1], pr.at[k, 1], d_xm)

    def xb(k):
        got(XA.at[k, 0], pr.at[k, 0])
        PS[xp, t[k], 0] = (PS[xp, t[k], 0].astype(F32) + XA[k, 0].astype(F32)).astype(BF)
        go(PS.at[xp, t[k]], XB.at[k, 0], ps.at[k, 2], pr.at[k, 2], d_xp)
        got(XA.at[k, 1], pr.at[k, 1])
        PS[xm, t[k], 1] = (PS[xm, t[k], 1].astype(F32) + XA[k, 1].astype(F32)).astype(BF)
        go(PS.at[xm, t[k]], XB.at[k, 1], ps.at[k, 3], pr.at[k, 3], d_xm)

    def x_got(k):
        got(XB.at[k, 0], pr.at[k, 2])
        got(XB.at[k, 1], pr.at[k, 3])

    def x_sum(k):
        return PS[x, t[k]].astype(F32) + XB[k, 0].astype(F32) + XB[k, 1].astype(F32)

    def ya(i, q):
        go(PF.at[q * 4 + yo, 0], YA.at[i, 0], fs.at[i, 0], fr.at[i, 0], d_yp)
        go(PF.at[q * 4 + yo, 1], YA.at[i, 1], fs.at[i, 1], fr.at[i, 1], d_ym)

    def yb(i, q):
        got(YA.at[i, 0], fr.at[i, 0])
        PF[q * 4 + yp, 0] = (PF[q * 4 + yp, 0].astype(F32) + YA[i, 0].astype(F32)).astype(BF)
        go(PF.at[q * 4 + yp], YB.at[i, 0], fs.at[i, 2], fr.at[i, 2], d_yp)
        got(YA.at[i, 1], fr.at[i, 1])
        PF[q * 4 + ym, 1] = (PF[q * 4 + ym, 1].astype(F32) + YA[i, 1].astype(F32)).astype(BF)
        go(PF.at[q * 4 + ym], YB.at[i, 1], fs.at[i, 3], fr.at[i, 3], d_ym)

    def y_sum(i, q):
        got(YB.at[i, 0], fr.at[i, 2])
        got(YB.at[i, 1], fr.at[i, 3])
        return PF[q * 4 + y].astype(F32) + YB[i, 0].astype(F32) + YB[i, 1].astype(F32)

    def z_end(k):
        @pl.when(mid == 0)
        def _():
            SZ[k] = x_sum(k).astype(BF)
            go_if(0, SZ.at[k], ZO.at[2 - k], ss, k, sr.at[2 - k], d_in)

    def z_mid(k):
        @pl.when(mid == 1)
        def _():
            buf, slot = ((ZO.at[2], 2), (ZO.at[1], 1), (ZI.at[1], 4))[k]
            got(buf, sr.at[slot])
            SZ[k] = (x_sum(k) + buf[...].astype(F32)).astype(BF)
            to, d = ((1, d_in), (0, d_in), (0, d_out))[k]
            go_if(1, SZ.at[k], ZI.at[to], ss, k, sr.at[3 + to], d)

    xa(0)
    xa(1)
    gs_task(xp)
    gs_task(xm)
    x_end(2)
    x_end(3)
    gf_task(1 - first)
    ya(0, 1 - zh)
    ya(1, zh)
    xb(0)
    xa(2)
    yb(0, 1 - zh)
    xb(1)
    xa(3)
    gs_task(x)
    yb(1, zh)
    x_got(0)
    z_end(0)
    TZ[...] = y_sum(0, 1 - zh).astype(BF)
    go(TZ, ZH, es.at[1], er.at[1], d_zh)
    xb(2)
    z_mid(0)
    x_got(1)
    z_end(1)
    xb(3)
    z_mid(1)
    own = y_sum(1, zh)
    got(ZH, er.at[1])
    FS[...] = (own + ZH[...].astype(F32)).astype(BF)
    go(FS.at[1 - c], FX, cs.at[5], cr.at[5], d_core)
    gf_ref[:, c] = FS[c]
    x_got(2)
    z_end(2)
    z_mid(2)
    got(FX, cr.at[5])
    gf_ref[:, 1 - c] = FX[...]
    x_got(3)
    got(ZI.at[0], sr.at[3])

    @pl.when(mid == 0)
    def _():
        r = (x_sum(3) + ZI[0].astype(F32)).astype(BF)
        gs_ref[:, pl.ds(0, 1024)] = r[0]
        gs_ref[:, pl.ds(1024, 1024)] = r[1]

    @pl.when(mid == 1)
    def _():
        got(ZO.at[0], sr.at[0])
        r = (x_sum(3) + ZI[0].astype(F32) + ZO[0].astype(F32)).astype(BF)
        gs_ref[:, pl.ds(0, 1024)] = r[0]
        gs_ref[:, pl.ds(1024, 1024)] = r[1]

    for cp in pending:
        cp.wait_send()
    for w in (0, 1):
        @pl.when(mid == w)
        def _():
            for when, sems, i in block_sends:
                if when == w:
                    rc(SZ.at[0], SZ.at[0], sems.at[i], sr.at[0], d_core).wait_send()


def local(embed_first, embed_second, corr_grad):
    dma = pltpu.SemaphoreType.DMA
    vm = pltpu.VMEM
    gf, gs = pl.pallas_call(
        kernel,
        out_shape=(jax.ShapeDtypeStruct((2, 2, 48, 512), BF), jax.ShapeDtypeStruct((48, 2048), BF)),
        in_specs=[pl.BlockSpec(memory_space=pl.ANY)] * 3,
        out_specs=[pl.BlockSpec(memory_space=pltpu.VMEM)] * 2,
        scratch_shapes=[
            vm((2, 2, 48, 512), BF),
            vm((8, 2, 2, 48, 512), BF),
            vm((4, 4, 2, 48, 1024), BF),
            vm((4, 128, 2048), F32),
            vm((2, 512, 2048), BF),
            vm((4, 4, 2, 48, 1024), BF),
            vm((8, 2, 2, 48, 512), BF),
            vm((4, 2, 48, 1024), BF),
            vm((4, 2, 2, 48, 1024), BF),
            vm((2, 2, 2, 48, 512), BF),
            vm((2, 2, 2, 2, 48, 512), BF),
            vm((3, 2, 48, 1024), BF),
            vm((2, 2, 48, 1024), BF),
            vm((3, 2, 48, 1024), BF),
            vm((2, 2, 48, 512), BF),
            vm((2, 2, 48, 512), BF),
            vm((2, 2, 48, 512), BF),
            vm((2, 48, 512), BF),
            dma((4,)), dma((4,)),
            dma((6,)), dma((6,)),
            dma((2,)), dma((2,)),
            dma((5,)), dma((4,)),
            dma((2, 4)), dma((2, 4)),
            dma((4, 4)), dma((4, 4)),
            dma((4, 4)), dma((4, 4)),
            dma((2, 4)), dma((2, 4)),
            dma((3,)), dma((5,)),
        ],
        compiler_params=pltpu.CompilerParams(
            collective_id=0, has_side_effects=True, vmem_limit_bytes=60 * 2**20
        ),
    )(embed_first.reshape(2, 2, 48, 512), embed_second, corr_grad)
    return gf.reshape(192, 512), gs


def solution(mesh):
    return jax.shard_map(
        local,
        mesh=mesh,
        in_specs=(P("col", "row"), P("row", "col"), P("row", "col")),
        out_specs=(P("col", "row"), P("row", "col")),
        check_vma=False,
    )
```

```python
import jax
import jax.numpy as jnp
from jax import lax
from jax.experimental import pallas as pl
from jax.experimental.pallas import tpu as pltpu
from jax.sharding import PartitionSpec as P

BF = jnp.bfloat16
F32 = jnp.float32
MESH = pl.DeviceIdType.MESH


def kernel(e1_hbm, e2_hbm, g_hbm, gf_ref, gs_ref,
           e1s, E1, E2, gst, G, PS, PF, XA, XB, YA, YB, ZO, ZI, SZ, TZ, ZH, FS, FX,
           lsem, gsem, cs, cr, es, er, zs, zr, ys, yr, xs, xr, ps, pr, fs, fr, ss, sr):
    row = lax.axis_index("row")
    col = lax.axis_index("col")
    x, p, c = row // 8, (row // 2) % 4, row % 2
    zh, y = col // 4, col % 4
    s = 1 - 2 * (p // 2)
    mid = ((p + 1) // 2) % 2
    first = p // 2

    def dev(x_=x, p_=p, c_=c, zh_=zh, y_=y):
        return ((x_ * 4 + p_) * 2 + c_, zh_ * 4 + y_)

    xp, xm, xo = (x + 1) % 4, (x + 3) % 4, (x + 2) % 4
    yp, ym, yo = (y + 1) % 4, (y + 3) % 4, (y + 2) % 4
    d_core = dev(c_=1 - c)
    d_xp, d_xm = dev(x_=xp), dev(x_=xm)
    d_yp, d_ym = dev(y_=yp), dev(y_=ym)
    d_zh = dev(zh_=1 - zh)
    d_in = dev(p_=p + s)
    d_out = dev(p_=(p - s + 4) % 4)

    sends, side = [], [0]

    def rc(src, dst, ssem, rsem, d):
        return pltpu.make_async_remote_copy(src, dst, ssem, rsem, device_id=d, device_id_type=MESH)

    def go(src, dst, sems, i, rsem, d):
        go_if(None, src, dst, sems, i, rsem, d)

    def go_if(when, src, dst, sems, i, rsem, d):
        rc(src, dst, sems.at[i], rsem, d).start()
        if not any(w == when and a is sems and b == i for w, a, b in sends):
            sends.append((when, sems, i))

    def got(dst, rsem):
        rc(dst, dst, rsem, rsem, d_core).wait_recv()

    o = [p + s * (mid * m + (1 - mid) * e) for m, e in ((0, 0), (-1, 1), (1, 2), (2, 3))]
    t = [p + s * (mid * m + (1 - mid) * e) for m, e in ((2, 3), (1, 2), (-1, 1), (0, 0))]

    l2 = [pltpu.make_async_copy(e2_hbm.at[:, pl.ds(h * 1024, 1024)], E2.at[p, x, h], lsem.at[h]) for h in range(2)]
    l1 = pltpu.make_async_copy(e1_hbm, e1s, lsem.at[2])
    l1own = pltpu.make_async_copy(e1_hbm.at[:, c], E1.at[col, c], lsem.at[3])
    for cp in l2:
        cp.start()
    l1.start()
    l1own.start()
    lg = [pltpu.make_async_copy(g_hbm.at[pl.ds(i * 128, 128)], gst.at[i], gsem.at[i]) for i in range(4)]
    for cp in lg:
        cp.start()

    barrier = pltpu.get_barrier_semaphore()
    for d in (d_core, d_xp, d_xm, d_yp, d_ym, d_zh, d_in):
        pl.semaphore_signal(barrier, 1, device_id=d, device_id_type=MESH)

    @pl.when(mid == 1)
    def _():
        pl.semaphore_signal(barrier, 1, device_id=d_out, device_id_type=MESH)

    pl.semaphore_wait(barrier, 7 + mid)

    for cp in l2:
        cp.wait()

    @pl.when(mid == 1)
    def _():
        for h in range(2):
            go_if(1, E2.at[p, x, h], E2.at[p, x, h], zs, (0, h), zr.at[0, h], d_in)
            go_if(1, E2.at[p, x, h], E2.at[p, x, h], zs, (1, h), zr.at[0, h], d_out)

    @pl.when(mid == 0)
    def _():
        for h in range(2):
            go_if(0, E2.at[p, x, h], E2.at[p, x, h], zs, (0, h), zr.at[3, h], d_in)

    def x_send(k, r, h):
        go(E2.at[o[k], x, h], E2.at[o[k], x, h], xs, (k, r, h,), xr.at[k, r, h], (d_xp, d_xm)[r])

    def x_fwd(k):
        for r, frm, to in ((0, xm, d_xp), (1, xp, d_xm)):
            got(E2.at[o[k], frm, r], xr.at[k, r, r])
            go(E2.at[o[k], frm, r], E2.at[o[k], frm, r], xs, (k, 2, r,), xr.at[k, 2, r], to)

    def x_end(k):
        got(E2.at[o[k], xm, 1], xr.at[k, 0, 1])
        got(E2.at[o[k], xp, 0], xr.at[k, 1, 0])
        got(E2.at[o[k], xo, 0], xr.at[k, 2, 0])
        got(E2.at[o[k], xo, 1], xr.at[k, 2, 1])

    zslot = [None] + [mid * m + (1 - mid) * e for m, e in ((3, 0), (0, 1), (1, 2))]

    def z_step(k, h):
        got(E2.at[o[k], x, h], zr.at[zslot[k], h])
        x_send(k, 0, h)
        x_send(k, 1, h)

        if side[0]:
            d = d_in if k == 1 else d_out
            slot = 1 if k < 3 else 2
            go_if(1, E2.at[o[k], x, h], E2.at[o[k], x, h], zs, (k + 1, h), zr.at[slot, h], d)

    for r, h in ((0, 0), (1, 1), (0, 1), (1, 0)):
        x_send(0, r, h)

    l1.wait()
    go(e1s.at[:, 1 - c], E1.at[col, c], cs, (0,), cr.at[0], d_core)
    l1own.wait()
    got(E1.at[col, 1 - c], cr.at[0])

    def y_send(i, q, r, h):
        b = q * 4 + y
        go(E1.at[b, h], E1.at[b, h], ys, (i, r, h,), yr.at[i, r, h], (d_yp, d_ym)[r])

    def y_fwd(i, q):
        for r, frm, to in ((0, q * 4 + ym, d_yp), (1, q * 4 + yp, d_ym)):
            got(E1.at[frm, r], yr.at[i, r, r])
            go(E1.at[frm, r], E1.at[frm, r], ys, (i, 2, r,), yr.at[i, 2, r], to)

    def y_end(i, q):
        got(E1.at[q * 4 + ym, 1], yr.at[i, 0, 1])
        got(E1.at[q * 4 + yp, 0], yr.at[i, 1, 0])
        got(E1.at[q * 4 + yo, 0], yr.at[i, 2, 0])
        got(E1.at[q * 4 + yo, 1], yr.at[i, 2, 1])

    for r, h in ((0, 0), (1, 1), (0, 1), (1, 0)):
        y_send(0, zh, r, h)

    def zh_send():
        for h in range(2):
            go(E1.at[col, h], E1.at[col, h], es, (0, h,), er.at[0, h], d_zh)

    def zh_got(h):
        got(E1.at[(1 - zh) * 4 + y, h], er.at[0, h])
        y_send(1, 1 - zh, 0, h)
        y_send(1, 1 - zh, 1, h)

    for i in range(4):
        lg[i].wait()
        G[c, pl.ds(i * 128, 128), :] = gst[i].astype(BF)
        go(G.at[c, pl.ds(i * 128, 128)], G.at[c, pl.ds(i * 128, 128)], cs, (1 + i,), cr.at[1 + i], d_core)

    def g_got():
        for i in range(4):
            got(G.at[1 - c, pl.ds(i * 128, 128)], cr.at[1 + i])

    def gf_task(k):
        ok = o[k]
        a, i = ok // 2, ok % 2

        def body(h, carry):
            acc = None
            for hj in range(2):
                lhs = E2[ok, :, hj].reshape(192, 1024)
                r = lax.dot_general(lhs, G[h, :, pl.ds(hj * 1024, 1024)], (((1,), (1,)), ((), ())),
                                    preferred_element_type=F32)
                acc = r if acc is None else acc + r
            acc = acc.astype(BF).reshape(4, 48, 512)
            for n in range(4):
                PF[2 * n + a, h, i] = acc[n]
            return carry
        lax.fori_loop(0, 2, body, 0)

    def gs_task(xx):
        def body(n, carry):
            acc = None
            for h in range(2):
                lhs = E1[pl.ds(2 * xx, 2), h].reshape(192, 512)
                r = jnp.dot(lhs, G[h, :, pl.ds(pl.multiple_of(n * 512, 512), 512)], preferred_element_type=F32)
                acc = r if acc is None else acc + r
            PS[xx, :, n // 2, :, pl.ds(pl.multiple_of((n % 2) * 512, 512), 512)] = acc.astype(BF).reshape(4, 48, 512)
            return carry
        lax.fori_loop(0, 4, body, 0)

    def xa(k):
        for r, d in ((0, d_xp), (1, d_xm)):
            go(PS.at[xo, t[k], r], XA.at[k, r], ps, (k, 0, r,), pr.at[k, 0, r], d)

    def xb(k):
        for r, n, d in ((0, xp, d_xp), (1, xm, d_xm)):
            go(PS.at[n, t[k], 1 - r], XB.at[k, r, 1 - r], ps, (k, 1, r,), pr.at[k, 1, r], d)

    def xc(k):
        for r, n, d in ((0, xp, d_xp), (1, xm, d_xm)):
            got(XA.at[k, r], pr.at[k, 0, r])
            PS[n, t[k], r] = (PS[n, t[k], r].astype(F32) + XA[k, r].astype(F32)).astype(BF)
            go(PS.at[n, t[k], r], XB.at[k, r, r], ps, (k, 2, r,), pr.at[k, 2, r], d)

    def x_got(k):
        for r in range(2):
            got(XB.at[k, r, 1 - r], pr.at[k, 1, r])
            got(XB.at[k, r, r], pr.at[k, 2, r])

    def x_sum(k, h):
        return PS[x, t[k], h].astype(F32) + XB[k, 0, h].astype(F32) + XB[k, 1, h].astype(F32)

    def ya(i, q):
        for r, d in ((0, d_yp), (1, d_ym)):
            go(PF.at[q * 4 + yo, r], YA.at[i, r], fs, (i, 0, r,), fr.at[i, 0, r], d)

    def yb(i, q):
        for r, n, d in ((0, yp, d_yp), (1, ym, d_ym)):
            go(PF.at[q * 4 + n, 1 - r], YB.at[i, r, 1 - r], fs, (i, 1, r,), fr.at[i, 1, r], d)

    def yc(i, q):
        for r, n, d in ((0, yp, d_yp), (1, ym, d_ym)):
            got(YA.at[i, r], fr.at[i, 0, r])
            PF[q * 4 + n, r] = (PF[q * 4 + n, r].astype(F32) + YA[i, r].astype(F32)).astype(BF)
            go(PF.at[q * 4 + n, r], YB.at[i, r, r], fs, (i, 2, r,), fr.at[i, 2, r], d)

    def y_sum(i, q):
        for r in range(2):
            got(YB.at[i, r, 1 - r], fr.at[i, 1, r])
            got(YB.at[i, r, r], fr.at[i, 2, r])
        return PF[q * 4 + y].astype(F32) + YB[i, 0].astype(F32) + YB[i, 1].astype(F32)

    def z_end(k):
        for h in range(2):
            SZ[k, h] = x_sum(k, h).astype(BF)
            go_if(0, SZ.at[k, h], ZO.at[2 - k, h], ss, (k, h), sr.at[2 - k, h], d_in)

    def z_mid(k, h):
        buf, slot = ((ZO.at[2], 2), (ZO.at[1], 1), (ZI.at[1], 4))[k]
        got(buf.at[h], sr.at[slot, h])
        SZ[k, h] = (x_sum(k, h) + buf[h].astype(F32)).astype(BF)
        to, d = ((1, d_in), (0, d_in), (0, d_out))[k]
        go_if(1, SZ.at[k, h], ZI.at[to, h], ss, (k, h), sr.at[3 + to, h], d)

    def tz():
        TZ[...] = y_sum(0, 1 - zh).astype(BF)
        for h in range(2):
            go(TZ.at[h], ZH.at[h], es, (1, h,), er.at[1, h], d_zh)

    def own(cl, f, *a):
        @pl.when((y + cl) % 2 == 0)
        def _():
            f(*a)

    def relay(cl, f, *a):
        @pl.when((y + cl) % 2 == 1)
        def _():
            f(*a)

    def gf_end():
        mine = y_sum(1, zh)
        for h in range(2):
            got(ZH.at[h], er.at[1, h])
        FS[...] = (mine + ZH[...].astype(F32)).astype(BF)
        go(FS.at[1 - c], FX, cs, (5,), cr.at[5], d_core)
        gf_ref[:, c] = FS[c]

    def gf_out():
        got(FX, cr.at[5])
        gf_ref[:, 1 - c] = FX[...]

    def gs_out(h):
        got(ZI.at[0, h], sr.at[3, h])

        total = x_sum(3, h) + ZI[0, h].astype(F32)
        if side[0]:
            got(ZO.at[0, h], sr.at[0, h])
            total = total + ZO[0, h].astype(F32)
        gs_ref[:, pl.ds(h * 1024, 1024)] = total.astype(BF)

    early = 2 * zh
    late = 2 * (1 - zh)
    odd = xo % 2

    def run(*steps):
        for f, *a in steps:
            with jax.named_scope(f.__name__ + "_".join(getattr(v, "__name__", str(v)) if isinstance(v, int) or callable(v) else "v" for v in a)):
                f(*a)

    def finish(w):
        for when, sems, i in sends:
            if when is None or when == w:
                like = G.at[0, pl.ds(0, 128)] if sems is cs and 1 <= i[0] <= 4 else SZ.at[0, 0]
                rc(like, like, sems.at[i], sr.at[0, 0], d_core).wait_send()

    @pl.when(mid == 0)
    def _():
        side[0] = 0
        run(
            (zh_send,), (x_fwd, 0), (z_step, 1, 0), (y_fwd, 0, zh), (z_step, 1, 1), (x_fwd, 1), (zh_got, 0),
            (x_end, 0), (g_got,), (gf_task, 0), (zh_got, 1), (y_end, 0, zh), (gs_task, early), (z_step, 2, 0), (z_step, 2, 1),
            (y_fwd, 1, 1 - zh), (x_end, 1), (gf_task, 1), (own, first, ya, 0, 1 - zh), (relay, first, yb, 0, 1 - zh), (own, first, ya, 1, zh),
            (x_fwd, 2), (z_step, 3, 0), (z_step, 3, 1), (gs_task, early + 1),
            (y_end, 1, 1 - zh), (gs_task, late + odd), (xa, 0), (relay, first, yc, 0, 1 - zh), (gs_task, late + 1 - odd),
            (relay, first, yb, 1, zh), (relay, first, yc, 1, zh),
            (x_end, 2), (gf_task, 2), (x_fwd, 3), (xb, 0), (xc, 0), (xa, 1), (xb, 1), (xa, 2), (own, first, tz),
            (x_end, 3), (gf_task, 3), (own, 1 - first, ya, 0, 1 - zh), (relay, 1 - first, yb, 0, 1 - zh), (own, 1 - first, ya, 1, zh),
            (xc, 1), (xb, 2), (xa, 3), (x_got, 0), (z_end, 0),
            (relay, 1 - first, yc, 0, 1 - zh), (relay, 1 - first, yb, 1, zh), (relay, 1 - first, yc, 1, zh),
            (xc, 2), (xb, 3), (own, 1 - first, tz), (x_got, 1), (z_end, 1), (xc, 3),
            (x_got, 2), (z_end, 2), (gf_end,), (gf_out,),
            (x_got, 3), (gs_out, 0), (gs_out, 1),
        )
        finish(0)

    @pl.when(mid == 1)
    def _():
        side[0] = 1
        run(
            (zh_send,), (x_fwd, 0), (z_step, 1, 0), (z_step, 2, 0), (y_fwd, 0, zh), (z_step, 1, 1), (z_step, 2, 1),
            (x_end, 0), (g_got,), (gf_task, 0), (z_step, 3, 0), (zh_got, 0), (z_step, 3, 1), (zh_got, 1), (x_fwd, 1),
            (y_end, 0, zh), (gs_task, early), (x_fwd, 2), (y_fwd, 1, 1 - zh), (x_end, 1), (gf_task, 1),
            (own, first, ya, 0, 1 - zh), (relay, first, yb, 0, 1 - zh), (own, first, ya, 1, zh), (gs_task, early + 1),
            (x_fwd, 3), (y_end, 1, 1 - zh), (gs_task, late + odd), (xa, 0), (relay, first, yc, 0, 1 - zh), (gs_task, late + 1 - odd), (xb, 0),
            (xa, 1), (relay, first, yb, 1, zh), (relay, first, yc, 1, zh),
            (x_end, 2), (gf_task, 2), (xc, 0), (xb, 1), (xa, 2),
            (x_end, 3), (gf_task, 3), (own, 1 - first, ya, 0, 1 - zh), (relay, 1 - first, yb, 0, 1 - zh), (own, 1 - first, ya, 1, zh),
            (own, first, tz),
            (xc, 1), (xb, 2), (xa, 3), (x_got, 0),
            (relay, 1 - first, yc, 0, 1 - zh), (relay, 1 - first, yb, 1, zh), (relay, 1 - first, yc, 1, zh), (xc, 2), (xb, 3),
            (z_mid, 0, 0), (z_mid, 0, 1), (own, 1 - first, tz), (xc, 3), (x_got, 1),
            (z_mid, 1, 0), (z_mid, 1, 1), (x_got, 2), (z_mid, 2, 0), (z_mid, 2, 1), (gf_end,), (gf_out,),
            (x_got, 3), (gs_out, 0), (gs_out, 1),
        )
        finish(1)


def local(embed_first, embed_second, corr_grad):
    dma = pltpu.SemaphoreType.DMA
    vm = pltpu.VMEM
    hbm = lambda a: pltpu.with_memory_space_constraint(a, pltpu.HBM)
    gf, gs = pl.pallas_call(
        kernel,
        out_shape=(jax.ShapeDtypeStruct((2, 2, 48, 512), BF), jax.ShapeDtypeStruct((48, 2048), BF)),
        in_specs=[pl.BlockSpec(memory_space=pl.ANY)] * 3,
        out_specs=[pl.BlockSpec(memory_space=pltpu.VMEM)] * 2,
        scratch_shapes=[
            vm((2, 2, 48, 512), BF),
            vm((8, 2, 2, 48, 512), BF),
            vm((4, 4, 2, 48, 1024), BF),
            vm((4, 128, 2048), F32),
            vm((2, 512, 2048), BF),
            vm((4, 4, 2, 48, 1024), BF),
            vm((8, 2, 2, 48, 512), BF),
            vm((4, 2, 48, 1024), BF),
            vm((4, 2, 2, 48, 1024), BF),
            vm((2, 2, 2, 48, 512), BF),
            vm((2, 2, 2, 2, 48, 512), BF),
            vm((3, 2, 48, 1024), BF),
            vm((2, 2, 48, 1024), BF),
            vm((3, 2, 48, 1024), BF),
            vm((2, 2, 48, 512), BF),
            vm((2, 2, 48, 512), BF),
            vm((2, 2, 48, 512), BF),
            vm((2, 48, 512), BF),
            dma((4,)), dma((4,)),
            dma((6,)), dma((6,)),
            dma((2, 2)), dma((2, 2)),
            dma((5, 2)), dma((4, 2)),
            dma((2, 3, 2)), dma((2, 3, 2)),
            dma((4, 3, 2)), dma((4, 3, 2)),
            dma((4, 3, 2)), dma((4, 3, 2)),
            dma((2, 3, 2)), dma((2, 3, 2)),
            dma((3, 2)), dma((5, 2)),
        ],
        compiler_params=pltpu.CompilerParams(
            collective_id=0, has_side_effects=True, vmem_limit_bytes=50 * 2**20
        ),
    )(hbm(embed_first.reshape(2, 2, 48, 512)), hbm(embed_second), hbm(corr_grad))
    return gf.reshape(192, 512), gs


def solution(mesh):
    return jax.shard_map(
        local,
        mesh=mesh,
        in_specs=(P("col", "row"), P("row", "col"), P("row", "col")),
        out_specs=(P("col", "row"), P("row", "col")),
        check_vma=False,
    )
```

```python
import jax
import jax.numpy as jnp
from jax import lax
from jax.experimental import pallas as pl
from jax.experimental.pallas import tpu as pltpu
from jax.sharding import PartitionSpec as P

BF = jnp.bfloat16
F32 = jnp.float32
MESH = pl.DeviceIdType.MESH


def kernel(e1_hbm, e2_hbm, g_hbm, gf_ref, gs_ref,
           e1s, E1, E2, gst, G, PS, PF, XA, XB, YA, YB, ZO, ZI, SZ, TZ, ZH, FS, FX,
           lsem, gsem, cs, cr, es, er, zs, zr, ys, yr, xs, xr, ps, pr, fs, fr, ss, sr):
    row = lax.axis_index("row")
    col = lax.axis_index("col")
    x, p, c = row // 8, (row // 2) % 4, row % 2
    zh, y = col // 4, col % 4
    s = 1 - 2 * (p // 2)
    mid = ((p + 1) // 2) % 2
    first = p // 2

    def dev(x_=x, p_=p, c_=c, zh_=zh, y_=y):
        return ((x_ * 4 + p_) * 2 + c_, zh_ * 4 + y_)

    xp, xm, xo = (x + 1) % 4, (x + 3) % 4, (x + 2) % 4
    yp, ym, yo = (y + 1) % 4, (y + 3) % 4, (y + 2) % 4
    d_core = dev(c_=1 - c)
    d_xp, d_xm = dev(x_=xp), dev(x_=xm)
    d_yp, d_ym = dev(y_=yp), dev(y_=ym)
    d_zh = dev(zh_=1 - zh)
    d_in = dev(p_=p + s)
    d_out = dev(p_=(p - s + 4) % 4)

    sends, side = [], [0]

    def rc(src, dst, ssem, rsem, d):
        return pltpu.make_async_remote_copy(src, dst, ssem, rsem, device_id=d, device_id_type=MESH)

    def go(src, dst, sems, i, rsem, d):
        go_if(None, src, dst, sems, i, rsem, d)

    def go_if(when, src, dst, sems, i, rsem, d):
        rc(src, dst, sems.at[i], rsem, d).start()
        if not any(w == when and a is sems and b == i for w, a, b in sends):
            sends.append((when, sems, i))

    def got(dst, rsem):
        rc(dst, dst, rsem, rsem, d_core).wait_recv()

    o = [p + s * (mid * m + (1 - mid) * e) for m, e in ((0, 0), (-1, 1), (1, 2), (2, 3))]
    t = [p + s * (mid * m + (1 - mid) * e) for m, e in ((2, 3), (1, 2), (-1, 1), (0, 0))]

    l2 = [pltpu.make_async_copy(e2_hbm.at[:, pl.ds(h * 1024, 1024)], E2.at[p, x, h], lsem.at[h]) for h in range(2)]
    l1 = pltpu.make_async_copy(e1_hbm, e1s, lsem.at[2])
    l1own = pltpu.make_async_copy(e1_hbm.at[:, c], E1.at[col, :, c], lsem.at[3])
    for cp in l2:
        cp.start()
    l1.start()
    l1own.start()
    lg = [pltpu.make_async_copy(g_hbm.at[pl.ds(i * 128, 128)], gst.at[i], gsem.at[i]) for i in range(4)]
    for cp in lg:
        cp.start()

    barrier = pltpu.get_barrier_semaphore()
    for d in (d_core, d_xp, d_xm, d_yp, d_ym, d_zh, d_in):
        pl.semaphore_signal(barrier, 1, device_id=d, device_id_type=MESH)

    @pl.when(mid == 1)
    def _():
        pl.semaphore_signal(barrier, 1, device_id=d_out, device_id_type=MESH)

    pl.semaphore_wait(barrier, 7 + mid)

    for cp in l2:
        cp.wait()

    @pl.when(mid == 1)
    def _():
        for h in range(2):
            go_if(1, E2.at[p, x, h], E2.at[p, x, h], zs, (0, h), zr.at[0, h], d_in)
            go_if(1, E2.at[p, x, h], E2.at[p, x, h], zs, (1, h), zr.at[0, h], d_out)

    @pl.when(mid == 0)
    def _():
        for h in range(2):
            go_if(0, E2.at[p, x, h], E2.at[p, x, h], zs, (0, h), zr.at[3, h], d_in)

    def x_send(k, r, h):
        go(E2.at[o[k], x, h], E2.at[o[k], x, h], xs, (k, r, h,), xr.at[k, r, h], (d_xp, d_xm)[r])

    def x_fwd(k):
        for r, frm, to in ((0, xm, d_xp), (1, xp, d_xm)):
            got(E2.at[o[k], frm, r], xr.at[k, r, r])
            go(E2.at[o[k], frm, r], E2.at[o[k], frm, r], xs, (k, 2, r,), xr.at[k, 2, r], to)

    def x_end(k):
        got(E2.at[o[k], xm, 1], xr.at[k, 0, 1])
        got(E2.at[o[k], xp, 0], xr.at[k, 1, 0])
        got(E2.at[o[k], xo, 0], xr.at[k, 2, 0])
        got(E2.at[o[k], xo, 1], xr.at[k, 2, 1])

    zslot = [None] + [mid * m + (1 - mid) * e for m, e in ((3, 0), (0, 1), (1, 2))]

    def x_out(k, h):
        x_send(k, 0, h)
        x_send(k, 1, h)

    def z_step(k, h, out=1):
        got(E2.at[o[k], x, h], zr.at[zslot[k], h])
        if out:
            x_out(k, h)

        if side[0]:
            d = d_in if k == 1 else d_out
            slot = 1 if k < 3 else 2
            go_if(1, E2.at[o[k], x, h], E2.at[o[k], x, h], zs, (k + 1, h), zr.at[slot, h], d)

    for r, h in ((0, 0), (1, 1), (0, 1), (1, 0)):
        x_send(0, r, h)

    l1.wait()
    go(e1s.at[:, 1 - c], E1.at[col, :, c], cs, (0,), cr.at[0], d_core)
    l1own.wait()
    got(E1.at[col, :, 1 - c], cr.at[0])

    w0 = (p + 1 + mid) % 2
    half = (w0, 1 - w0)

    def y_send(i, q, r, h):
        b = E1.at[q * 4 + y, half[h]]
        go(b, b, ys, (i, r, h), yr.at[i, r, h], (d_yp, d_ym)[r])

    def y_fwd(i, q, r):
        frm, to = ((q * 4 + ym, d_yp), (q * 4 + yp, d_ym))[r]
        got(E1.at[frm, half[r]], yr.at[i, r, r])
        go(E1.at[frm, half[r]], E1.at[frm, half[r]], ys, (i, 2, r), yr.at[i, 2, r], to)

    def y_end(i, q, h):
        got(E1.at[q * 4 + (yp, ym)[h], half[h]], yr.at[i, 1 - h, h])
        got(E1.at[q * 4 + yo, half[h]], yr.at[i, 2, h])

    for r, h in ((0, 0), (1, 1), (0, 1), (1, 0)):
        y_send(0, zh, r, h)

    def zh_send(*hs):
        for h in hs:
            b = E1.at[col, half[h]]
            go(b, b, es, (0, h), er.at[0, h], d_zh)

    def zh_got(h):
        got(E1.at[(1 - zh) * 4 + y, half[h]], er.at[0, h])
        y_send(1, 1 - zh, 0, h)
        y_send(1, 1 - zh, 1, h)

    for i in range(4):
        lg[i].wait()
        G[c, pl.ds(i * 128, 128), :] = gst[i].astype(BF)
        go(G.at[c, pl.ds(i * 128, 128)], G.at[c, pl.ds(i * 128, 128)], cs, (1 + i,), cr.at[1 + i], d_core)

    def g_got():
        for i in range(4):
            got(G.at[1 - c, pl.ds(i * 128, 128)], cr.at[1 + i])

    def gf_task(k):
        ok = o[k]
        a, i = ok // 2, ok % 2

        def body(h, carry):
            acc = None
            for hj in range(2):
                lhs = E2[ok, :, hj].reshape(192, 1024)
                r = lax.dot_general(lhs, G[h, :, pl.ds(hj * 1024, 1024)], (((1,), (1,)), ((), ())),
                                    preferred_element_type=F32)
                acc = r if acc is None else acc + r
            acc = acc.astype(BF).reshape(4, 48, 512)
            for n in range(4):
                PF[2 * n + a, h, i] = acc[n]
            return carry
        lax.fori_loop(0, 2, body, 0)

    def gs_task(q, w):
        def body(n, carry):
            acc = None
            for h in range(2):
                lhs = E1[pl.ds(4 * q, 4), half[w], h].reshape(192, 512)
                r = jnp.dot(lhs, G[h, :, pl.ds(pl.multiple_of(n * 512, 512), 512)], preferred_element_type=F32)
                acc = r if acc is None else acc + r
            acc = acc.astype(BF).reshape(4, 48, 512)
            for j in range(4):
                PS[2 * q + j // 2, 2 * (j % 2) + half[w], n // 2, :, pl.ds(pl.multiple_of((n % 2) * 512, 512), 512)] = acc[j]
            return carry
        lax.fori_loop(0, 4, body, 0)

    def xa(k):
        for r, d in ((0, d_xp), (1, d_xm)):
            go(PS.at[xo, t[k], r], XA.at[k, r], ps, (k, 0, r,), pr.at[k, 0, r], d)

    def xb(k):
        for r, n, d in ((0, xp, d_xp), (1, xm, d_xm)):
            go(PS.at[n, t[k], 1 - r], XB.at[k, r, 1 - r], ps, (k, 1, r,), pr.at[k, 1, r], d)

    def xc(k):
        for r, n, d in ((0, xp, d_xp), (1, xm, d_xm)):
            got(XA.at[k, r], pr.at[k, 0, r])
            PS[n, t[k], r] = (PS[n, t[k], r].astype(F32) + XA[k, r].astype(F32)).astype(BF)
            go(PS.at[n, t[k], r], XB.at[k, r, r], ps, (k, 2, r,), pr.at[k, 2, r], d)

    def x_got(k):
        for r in range(2):
            got(XB.at[k, r, 1 - r], pr.at[k, 1, r])
            got(XB.at[k, r, r], pr.at[k, 2, r])

    def x_sum(k, h):
        return PS[x, t[k], h].astype(F32) + XB[k, 0, h].astype(F32) + XB[k, 1, h].astype(F32)

    def ya(i, q):
        for r, d in ((0, d_yp), (1, d_ym)):
            go(PF.at[q * 4 + yo, r], YA.at[i, r], fs, (i, 0, r,), fr.at[i, 0, r], d)

    def yb(i, q):
        for r, n, d in ((0, yp, d_yp), (1, ym, d_ym)):
            go(PF.at[q * 4 + n, 1 - r], YB.at[i, r, 1 - r], fs, (i, 1, r,), fr.at[i, 1, r], d)

    def yc(i, q):
        for r, n, d in ((0, yp, d_yp), (1, ym, d_ym)):
            got(YA.at[i, r], fr.at[i, 0, r])
            PF[q * 4 + n, r] = (PF[q * 4 + n, r].astype(F32) + YA[i, r].astype(F32)).astype(BF)
            go(PF.at[q * 4 + n, r], YB.at[i, r, r], fs, (i, 2, r,), fr.at[i, 2, r], d)

    def y_sum(i, q):
        for r in range(2):
            got(YB.at[i, r, 1 - r], fr.at[i, 1, r])
            got(YB.at[i, r, r], fr.at[i, 2, r])
        return PF[q * 4 + y].astype(F32) + YB[i, 0].astype(F32) + YB[i, 1].astype(F32)

    def z_end(k):
        for h in range(2):
            SZ[k, h] = x_sum(k, h).astype(BF)
            go_if(0, SZ.at[k, h], ZO.at[2 - k, h], ss, (k, h), sr.at[2 - k, h], d_in)

    def z_mid(k, h):
        buf, slot = ((ZO.at[2], 2), (ZO.at[1], 1), (ZI.at[1], 4))[k]
        got(buf.at[h], sr.at[slot, h])
        SZ[k, h] = (x_sum(k, h) + buf[h].astype(F32)).astype(BF)
        to, d = ((1, d_in), (0, d_in), (0, d_out))[k]
        go_if(1, SZ.at[k, h], ZI.at[to, h], ss, (k, h), sr.at[3 + to, h], d)

    def tz():
        TZ[...] = y_sum(0, 1 - zh).astype(BF)
        for h in range(2):
            go(TZ.at[h], ZH.at[h], es, (1, h,), er.at[1, h], d_zh)

    def own(cl, f, *a):
        @pl.when((y + cl) % 2 == 0)
        def _():
            f(*a)

    def relay(cl, f, *a):
        @pl.when((y + cl) % 2 == 1)
        def _():
            f(*a)

    def gf_end():
        mine = y_sum(1, zh)
        for h in range(2):
            got(ZH.at[h], er.at[1, h])
        FS[...] = (mine + ZH[...].astype(F32)).astype(BF)
        go(FS.at[1 - c], FX, cs, (5,), cr.at[5], d_core)
        gf_ref[:, c] = FS[c]

    def gf_out():
        got(FX, cr.at[5])
        gf_ref[:, 1 - c] = FX[...]

    def gs_out(h):
        got(ZI.at[0, h], sr.at[3, h])

        total = x_sum(3, h) + ZI[0, h].astype(F32)
        if side[0]:
            got(ZO.at[0, h], sr.at[0, h])
            total = total + ZO[0, h].astype(F32)
        gs_ref[:, pl.ds(h * 1024, 1024)] = total.astype(BF)

    def run(*steps):
        for f, *a in steps:
            with jax.named_scope(f.__name__ + "_".join(getattr(v, "__name__", str(v)) if isinstance(v, int) or callable(v) else "v" for v in a)):
                f(*a)

    def finish(w):
        for when, sems, i in sends:
            if when is None or when == w:
                like = G.at[0, pl.ds(0, 128)] if sems is cs and 1 <= i[0] <= 4 else SZ.at[0, 0]
                rc(like, like, sems.at[i], sr.at[0, 0], d_core).wait_send()

    @pl.when(mid == 0)
    def _():
        side[0] = 0
        run(
            (zh_send, 0), (x_fwd, 0), (z_step, 1, 0), (y_fwd, 0, zh, 0), (y_fwd, 0, zh, 1), (z_step, 1, 1), (zh_got, 0),
            (x_end, 0), (g_got,), (gf_task, 0), (x_fwd, 1), (z_step, 2, 0), (y_end, 0, zh, 0), (gs_task, zh, 0), (z_step, 2, 1), (zh_send, 1),
            (y_fwd, 1, 1 - zh, 0), (x_end, 1), (gf_task, 1), (own, first, ya, 0, 1 - zh), (relay, first, yb, 0, 1 - zh), (own, first, ya, 1, zh),
            (z_step, 3, 0), (x_fwd, 2), (z_step, 3, 1), (zh_got, 1), (y_end, 1, 1 - zh, 0), (gs_task, 1 - zh, 0), (xa, 0),
            (relay, first, yc, 0, 1 - zh), (y_end, 0, zh, 1), (gs_task, zh, 1), (y_fwd, 1, 1 - zh, 1), (relay, first, yb, 1, zh),
            (x_end, 2), (gf_task, 2), (x_fwd, 3), (xb, 0), (xa, 2), (relay, first, yc, 1, zh), (own, first, tz),
            (y_end, 1, 1 - zh, 1), (gs_task, 1 - zh, 1), (xc, 0), (xa, 1), (xb, 1), (x_end, 3), (gf_task, 3),
            (own, 1 - first, ya, 0, 1 - zh), (relay, 1 - first, yb, 0, 1 - zh), (own, 1 - first, ya, 1, zh),
            (x_got, 0), (z_end, 0), (relay, 1 - first, yc, 0, 1 - zh), (relay, 1 - first, yb, 1, zh),
            (xc, 1), (xb, 2), (xc, 2), (xa, 3), (xb, 3), (relay, 1 - first, yc, 1, zh),
            (own, 1 - first, tz), (x_got, 1), (z_end, 1), (x_got, 2), (z_end, 2), (xc, 3),
            (gf_end,), (gf_out,),
            (x_got, 3), (gs_out, 0), (gs_out, 1),
        )
        finish(0)

    @pl.when(mid == 1)
    def _():
        side[0] = 1
        run(
            (zh_send, 0), (x_fwd, 0), (z_step, 1, 0), (y_fwd, 0, zh, 0), (y_fwd, 0, zh, 1), (z_step, 1, 1), (z_step, 2, 0), (z_step, 2, 1),
            (x_end, 0), (g_got,), (gf_task, 0), (zh_got, 0), (z_step, 3, 0, 0), (z_step, 3, 1, 0), (x_fwd, 1), (x_out, 3, 0), (x_out, 3, 1), (zh_send, 1),
            (y_end, 0, zh, 0), (gs_task, zh, 0), (y_fwd, 1, 1 - zh, 0), (x_fwd, 2), (y_end, 0, zh, 1), (gs_task, zh, 1),
            (x_end, 1), (gf_task, 1), (own, first, ya, 0, 1 - zh), (relay, first, yb, 0, 1 - zh), (own, first, ya, 1, zh),
            (zh_got, 1), (x_fwd, 3), (y_end, 1, 1 - zh, 0), (gs_task, 1 - zh, 0), (xa, 0), (xb, 0), (xa, 3),
            (relay, first, yc, 0, 1 - zh), (y_fwd, 1, 1 - zh, 1), (relay, first, yb, 1, zh), (x_end, 2), (gf_task, 2), (relay, first, yc, 1, zh),
            (x_end, 3), (gf_task, 3), (own, 1 - first, ya, 0, 1 - zh), (relay, 1 - first, yb, 0, 1 - zh), (own, 1 - first, ya, 1, zh),
            (xc, 0), (own, first, tz), (y_end, 1, 1 - zh, 1), (gs_task, 1 - zh, 1), (xa, 2), (xb, 2), (xa, 1),
            (relay, 1 - first, yc, 0, 1 - zh), (relay, 1 - first, yb, 1, zh), (relay, 1 - first, yc, 1, zh),
            (xc, 2), (xb, 1), (x_got, 0), (own, 1 - first, tz), (xc, 1), (xb, 3), (xc, 3),
            (z_mid, 0, 0), (z_mid, 0, 1), (x_got, 2), (z_mid, 2, 0), (z_mid, 2, 1), (x_got, 1), (z_mid, 1, 0), (z_mid, 1, 1),
            (gf_end,), (gf_out,),
            (x_got, 3), (gs_out, 0), (gs_out, 1),
        )
        finish(1)


def local(embed_first, embed_second, corr_grad):
    dma = pltpu.SemaphoreType.DMA
    vm = pltpu.VMEM
    hbm = lambda a: pltpu.with_memory_space_constraint(a, pltpu.HBM)
    gf, gs = pl.pallas_call(
        kernel,
        out_shape=(jax.ShapeDtypeStruct((2, 2, 48, 512), BF), jax.ShapeDtypeStruct((48, 2048), BF)),
        in_specs=[pl.BlockSpec(memory_space=pl.ANY)] * 3,
        out_specs=[pl.BlockSpec(memory_space=pltpu.VMEM)] * 2,
        scratch_shapes=[
            vm((2, 2, 48, 512), BF),
            vm((8, 2, 2, 48, 512), BF),
            vm((4, 4, 2, 48, 1024), BF),
            vm((4, 128, 2048), F32),
            vm((2, 512, 2048), BF),
            vm((4, 4, 2, 48, 1024), BF),
            vm((8, 2, 2, 48, 512), BF),
            vm((4, 2, 48, 1024), BF),
            vm((4, 2, 2, 48, 1024), BF),
            vm((2, 2, 2, 48, 512), BF),
            vm((2, 2, 2, 2, 48, 512), BF),
            vm((3, 2, 48, 1024), BF),
            vm((2, 2, 48, 1024), BF),
            vm((3, 2, 48, 1024), BF),
            vm((2, 2, 48, 512), BF),
            vm((2, 2, 48, 512), BF),
            vm((2, 2, 48, 512), BF),
            vm((2, 48, 512), BF),
            dma((4,)), dma((4,)),
            dma((6,)), dma((6,)),
            dma((2, 2)), dma((2, 2)),
            dma((5, 2)), dma((4, 2)),
            dma((2, 3, 2)), dma((2, 3, 2)),
            dma((4, 3, 2)), dma((4, 3, 2)),
            dma((4, 3, 2)), dma((4, 3, 2)),
            dma((2, 3, 2)), dma((2, 3, 2)),
            dma((3, 2)), dma((5, 2)),
        ],
        compiler_params=pltpu.CompilerParams(
            collective_id=0, has_side_effects=True, vmem_limit_bytes=50 * 2**20
        ),
    )(hbm(embed_first.reshape(2, 2, 48, 512)), hbm(embed_second), hbm(corr_grad))
    return gf.reshape(192, 512), gs


def solution(mesh):
    return jax.shard_map(
        local,
        mesh=mesh,
        in_specs=(P("col", "row"), P("row", "col"), P("row", "col")),
        out_specs=(P("col", "row"), P("row", "col")),
        check_vma=False,
    )
```

```python
import jax
import jax.numpy as jnp
from jax import lax
from jax.experimental import pallas as pl
from jax.experimental.pallas import tpu as pltpu
from jax.sharding import PartitionSpec as P

BF = jnp.bfloat16
F32 = jnp.float32
MESH = pl.DeviceIdType.MESH


def kernel(e1_hbm, e2_hbm, g_hbm, gf_ref, gs_ref,
           e1s, E1, E2, gst, G, PS, PF, XA, XB, YA, YB, ZO, ZI, SZ, TZ, ZH, FS, FX,
           lsem, gsem, cs, cr, es, er, zs, zr, ys, yr, xs, xr, ps, pr, fs, fr, ss, sr):
    row = lax.axis_index("row")
    col = lax.axis_index("col")
    x, p, c = row // 8, (row // 2) % 4, row % 2
    zh, y = col // 4, col % 4
    s = 1 - 2 * (p // 2)
    mid = ((p + 1) // 2) % 2
    first = p // 2

    def dev(x_=x, p_=p, c_=c, zh_=zh, y_=y):
        return ((x_ * 4 + p_) * 2 + c_, zh_ * 4 + y_)

    xp, xm, xo = (x + 1) % 4, (x + 3) % 4, (x + 2) % 4
    yp, ym, yo = (y + 1) % 4, (y + 3) % 4, (y + 2) % 4
    d_core = dev(c_=1 - c)
    d_xp, d_xm = dev(x_=xp), dev(x_=xm)
    d_yp, d_ym = dev(y_=yp), dev(y_=ym)
    d_zh = dev(zh_=1 - zh)
    d_in = dev(p_=p + s)
    d_out = dev(p_=(p - s + 4) % 4)

    sends, side = [], [0]

    def rc(src, dst, ssem, rsem, d):
        return pltpu.make_async_remote_copy(src, dst, ssem, rsem, device_id=d, device_id_type=MESH)

    def go(src, dst, sems, i, rsem, d):
        go_if(None, src, dst, sems, i, rsem, d)

    def go_if(when, src, dst, sems, i, rsem, d):
        rc(src, dst, sems.at[i], rsem, d).start()
        if not any(w == when and a is sems and b == i for w, a, b in sends):
            sends.append((when, sems, i))

    def got(dst, rsem):
        rc(dst, dst, rsem, rsem, d_core).wait_recv()

    o = [p + s * (mid * m + (1 - mid) * e) for m, e in ((0, 0), (-1, 1), (1, 2), (2, 3))]
    t = [p + s * (mid * m + (1 - mid) * e) for m, e in ((2, 3), (1, 2), (-1, 1), (0, 0))]

    l2 = [pltpu.make_async_copy(e2_hbm.at[:, pl.ds(h * 1024, 1024)], E2.at[p, x, h], lsem.at[h]) for h in range(2)]
    l1 = pltpu.make_async_copy(e1_hbm, e1s, lsem.at[2])
    l1own = pltpu.make_async_copy(e1_hbm.at[:, c], E1.at[col, :, c], lsem.at[3])
    for cp in l2:
        cp.start()
    l1.start()
    l1own.start()
    lg = [pltpu.make_async_copy(g_hbm.at[pl.ds(i * 128, 128)], gst.at[i], gsem.at[i]) for i in range(4)]

    barrier = pltpu.get_barrier_semaphore()
    for d in (d_core, d_xp, d_xm, d_yp, d_ym, d_zh, d_in):
        pl.semaphore_signal(barrier, 1, device_id=d, device_id_type=MESH)

    @pl.when(mid == 1)
    def _():
        pl.semaphore_signal(barrier, 1, device_id=d_out, device_id_type=MESH)

    pl.semaphore_wait(barrier, 7 + mid)

    for cp in l2:
        cp.wait()

    @pl.when(mid == 1)
    def _():
        for h in range(2):
            go_if(1, E2.at[p, x, h], E2.at[p, x, h], zs, (0, h), zr.at[0, h], d_in)
            go_if(1, E2.at[p, x, h], E2.at[p, x, h], zs, (1, h), zr.at[0, h], d_out)

    @pl.when(mid == 0)
    def _():
        for h in range(2):
            go_if(0, E2.at[p, x, h], E2.at[p, x, h], zs, (0, h), zr.at[3, h], d_in)

    def x_send(k, r, h):
        go(E2.at[o[k], x, h], E2.at[o[k], x, h], xs, (k, r, h,), xr.at[k, r, h], (d_xp, d_xm)[r])

    def x_fwd(k):
        for r, frm, to in ((0, xm, d_xp), (1, xp, d_xm)):
            got(E2.at[o[k], frm, r], xr.at[k, r, r])
            go(E2.at[o[k], frm, r], E2.at[o[k], frm, r], xs, (k, 2, r,), xr.at[k, 2, r], to)

    def x_end(k):
        got(E2.at[o[k], xm, 1], xr.at[k, 0, 1])
        got(E2.at[o[k], xp, 0], xr.at[k, 1, 0])
        got(E2.at[o[k], xo, 0], xr.at[k, 2, 0])
        got(E2.at[o[k], xo, 1], xr.at[k, 2, 1])

    zslot = [None] + [mid * m + (1 - mid) * e for m, e in ((3, 0), (0, 1), (1, 2))]

    def x_out(k, h):
        x_send(k, 0, h)
        x_send(k, 1, h)

    def z_step(k, h, out=1):
        got(E2.at[o[k], x, h], zr.at[zslot[k], h])
        if out:
            x_out(k, h)

        if side[0]:
            d = d_in if k == 1 else d_out
            slot = 1 if k < 3 else 2
            go_if(1, E2.at[o[k], x, h], E2.at[o[k], x, h], zs, (k + 1, h), zr.at[slot, h], d)

    for r, h in ((0, 0), (1, 1), (0, 1), (1, 0)):
        x_send(0, r, h)

    l1.wait()
    go(e1s.at[:, 1 - c], E1.at[col, :, c], cs, (0,), cr.at[0], d_core)
    for cp in lg:
        cp.start()
    l1own.wait()
    got(E1.at[col, :, 1 - c], cr.at[0])

    w0 = (p + 1 + mid) % 2
    half = (w0, 1 - w0)

    def y_send(i, q, r, h):
        b = E1.at[q * 4 + y, half[h]]
        go(b, b, ys, (i, r, h), yr.at[i, r, h], (d_yp, d_ym)[r])

    def y_fwd(i, q, r):
        frm, to = ((q * 4 + ym, d_yp), (q * 4 + yp, d_ym))[r]
        got(E1.at[frm, half[r]], yr.at[i, r, r])
        go(E1.at[frm, half[r]], E1.at[frm, half[r]], ys, (i, 2, r), yr.at[i, 2, r], to)

    def y_end(i, q, h):
        got(E1.at[q * 4 + (yp, ym)[h], half[h]], yr.at[i, 1 - h, h])
        got(E1.at[q * 4 + yo, half[h]], yr.at[i, 2, h])

    for r, h in ((0, 0), (1, 1), (0, 1), (1, 0)):
        y_send(0, zh, r, h)

    def zh_send(*hs):
        for h in hs:
            b = E1.at[col, half[h]]
            go(b, b, es, (0, h), er.at[0, h], d_zh)

    def zh_got(h):
        got(E1.at[(1 - zh) * 4 + y, half[h]], er.at[0, h])
        y_send(1, 1 - zh, 0, h)
        y_send(1, 1 - zh, 1, h)

    def g_share():
        for i in range(4):
            lg[i].wait()
            b = G.at[c, pl.ds(i * 128, 128)]
            G[c, pl.ds(i * 128, 128), :] = gst[i].astype(BF)
            go(b, b, cs, (1 + i,), cr.at[1 + i], d_core)

    def g_got():
        for i in range(4):
            got(G.at[1 - c, pl.ds(i * 128, 128)], cr.at[1 + i])

    def gf_task(k):
        ok = o[k]
        a, i = ok // 2, ok % 2

        def body(h, carry):
            acc = None
            for hj in range(2):
                lhs = E2[ok, :, hj].reshape(192, 1024)
                r = lax.dot_general(lhs, G[h, :, pl.ds(hj * 1024, 1024)], (((1,), (1,)), ((), ())),
                                    preferred_element_type=F32)
                acc = r if acc is None else acc + r
            acc = acc.astype(BF).reshape(4, 48, 512)
            for n in range(4):
                PF[2 * n + a, h, i] = acc[n]
            return carry
        lax.fori_loop(0, 2, body, 0)

    def gs_task(q, w):
        def body(n, carry):
            acc = None
            for h in range(2):
                lhs = E1[pl.ds(4 * q, 4), half[w], h].reshape(192, 512)
                r = jnp.dot(lhs, G[h, :, pl.ds(pl.multiple_of(n * 512, 512), 512)], preferred_element_type=F32)
                acc = r if acc is None else acc + r
            acc = acc.astype(BF).reshape(4, 48, 512)
            for j in range(4):
                PS[2 * q + j // 2, 2 * (j % 2) + half[w], n // 2, :, pl.ds(pl.multiple_of((n % 2) * 512, 512), 512)] = acc[j]
            return carry
        lax.fori_loop(0, 4, body, 0)

    def xa(k):
        for r, d in ((0, d_xp), (1, d_xm)):
            go(PS.at[xo, t[k], r], XA.at[k, r], ps, (k, 0, r,), pr.at[k, 0, r], d)

    def xb(k):
        for r, n, d in ((0, xp, d_xp), (1, xm, d_xm)):
            go(PS.at[n, t[k], 1 - r], XB.at[k, r, 1 - r], ps, (k, 1, r,), pr.at[k, 1, r], d)

    def xc(k):
        for r, n, d in ((0, xp, d_xp), (1, xm, d_xm)):
            got(XA.at[k, r], pr.at[k, 0, r])
            PS[n, t[k], r] = (PS[n, t[k], r].astype(F32) + XA[k, r].astype(F32)).astype(BF)
            go(PS.at[n, t[k], r], XB.at[k, r, r], ps, (k, 2, r,), pr.at[k, 2, r], d)

    def x_got(k):
        for r in range(2):
            got(XB.at[k, r, 1 - r], pr.at[k, 1, r])
            got(XB.at[k, r, r], pr.at[k, 2, r])

    def x_sum(k, h):
        return PS[x, t[k], h].astype(F32) + XB[k, 0, h].astype(F32) + XB[k, 1, h].astype(F32)

    def ya(i, q):
        for r, d in ((0, d_yp), (1, d_ym)):
            go(PF.at[q * 4 + yo, r], YA.at[i, r], fs, (i, 0, r,), fr.at[i, 0, r], d)

    def yb(i, q):
        for r, n, d in ((0, yp, d_yp), (1, ym, d_ym)):
            go(PF.at[q * 4 + n, 1 - r], YB.at[i, r, 1 - r], fs, (i, 1, r,), fr.at[i, 1, r], d)

    def yc(i, q):
        for r, n, d in ((0, yp, d_yp), (1, ym, d_ym)):
            got(YA.at[i, r], fr.at[i, 0, r])
            PF[q * 4 + n, r] = (PF[q * 4 + n, r].astype(F32) + YA[i, r].astype(F32)).astype(BF)
            go(PF.at[q * 4 + n, r], YB.at[i, r, r], fs, (i, 2, r,), fr.at[i, 2, r], d)

    def y_sum(i, q):
        for r in range(2):
            got(YB.at[i, r, 1 - r], fr.at[i, 1, r])
            got(YB.at[i, r, r], fr.at[i, 2, r])
        return PF[q * 4 + y].astype(F32) + YB[i, 0].astype(F32) + YB[i, 1].astype(F32)

    def z_end(k):
        for h in range(2):
            SZ[k, h] = x_sum(k, h).astype(BF)
            go_if(0, SZ.at[k, h], ZO.at[2 - k, h], ss, (k, h), sr.at[2 - k, h], d_in)

    def z_mid(k, h):
        buf, slot = ((ZO.at[2], 2), (ZO.at[1], 1), (ZI.at[1], 4))[k]
        got(buf.at[h], sr.at[slot, h])
        SZ[k, h] = (x_sum(k, h) + buf[h].astype(F32)).astype(BF)
        to, d = ((1, d_in), (0, d_in), (0, d_out))[k]
        go_if(1, SZ.at[k, h], ZI.at[to, h], ss, (k, h), sr.at[3 + to, h], d)

    def tz():
        TZ[...] = y_sum(0, 1 - zh).astype(BF)
        for h in range(2):
            go(TZ.at[h], ZH.at[h], es, (1, h,), er.at[1, h], d_zh)

    def own(cl, f, *a):
        @pl.when((y + cl) % 2 == 0)
        def _():
            f(*a)

    def relay(cl, f, *a):
        @pl.when((y + cl) % 2 == 1)
        def _():
            f(*a)

    def gf_end():
        mine = y_sum(1, zh)
        for h in range(2):
            got(ZH.at[h], er.at[1, h])
        FS[...] = (mine + ZH[...].astype(F32)).astype(BF)
        go(FS.at[1 - c], FX, cs, (5,), cr.at[5], d_core)
        gf_ref[:, c] = FS[c]

    def gf_out():
        got(FX, cr.at[5])
        gf_ref[:, 1 - c] = FX[...]

    def gs_out(h):
        got(ZI.at[0, h], sr.at[3, h])

        total = x_sum(3, h) + ZI[0, h].astype(F32)
        if side[0]:
            got(ZO.at[0, h], sr.at[0, h])
            total = total + ZO[0, h].astype(F32)
        gs_ref[:, pl.ds(h * 1024, 1024)] = total.astype(BF)

    def run(*steps):
        for f, *a in steps:
            with jax.named_scope(f.__name__ + "_".join(getattr(v, "__name__", str(v)) if isinstance(v, int) or callable(v) else "v" for v in a)):
                f(*a)

    def finish(w):
        for when, sems, i in sends:
            if when is None or when == w:
                like = G.at[0, pl.ds(0, 128)] if sems is cs and 1 <= i[0] <= 4 else SZ.at[0, 0]
                rc(like, like, sems.at[i], sr.at[0, 0], d_core).wait_send()

    @pl.when(mid == 0)
    def _():
        side[0] = 0
        run(
            (zh_send, 0), (g_share,), (x_fwd, 0), (z_step, 1, 0), (y_fwd, 0, zh, 0), (y_fwd, 0, zh, 1), (z_step, 1, 1), (zh_got, 0),
            (x_end, 0), (g_got,), (gf_task, 0), (x_fwd, 1), (z_step, 2, 0), (y_end, 0, zh, 0), (gs_task, zh, 0), (z_step, 2, 1), (zh_send, 1),
            (y_fwd, 1, 1 - zh, 0), (z_step, 3, 0), (x_end, 1), (gf_task, 1), (own, first, ya, 0, 1 - zh), (relay, first, yb, 0, 1 - zh),
            (z_step, 3, 1), (zh_got, 1), (x_fwd, 2), (y_end, 1, 1 - zh, 0), (gs_task, 1 - zh, 0), (xa, 0),
            (relay, first, yc, 0, 1 - zh), (y_end, 0, zh, 1), (gs_task, zh, 1), (x_fwd, 3), (xb, 0), (y_fwd, 1, 1 - zh, 1),
            (x_end, 2), (gf_task, 2), (own, first, tz), (xc, 0),
            (y_end, 1, 1 - zh, 1), (gs_task, 1 - zh, 1), (xa, 1), (xb, 1), (xa, 2), (x_end, 3), (gf_task, 3),
            (own, 1 - first, ya, 0, 1 - zh), (relay, 1 - first, yb, 0, 1 - zh), (own, first, ya, 1, zh), (relay, first, yb, 1, zh),
            (x_got, 0), (z_end, 0), (xc, 1), (xb, 2), (relay, 1 - first, yc, 0, 1 - zh), (relay, first, yc, 1, zh),
            (own, 1 - first, ya, 1, zh), (relay, 1 - first, yb, 1, zh), (xc, 2), (xa, 3), (xb, 3), (own, 1 - first, tz),
            (x_got, 1), (z_end, 1), (relay, 1 - first, yc, 1, zh), (x_got, 2), (z_end, 2), (xc, 3),
            (gf_end,), (gf_out,),
            (x_got, 3), (gs_out, 0), (gs_out, 1),
        )
        finish(0)

    @pl.when(mid == 1)
    def _():
        side[0] = 1
        run(
            (zh_send, 0), (g_share,), (x_fwd, 0), (z_step, 1, 0), (y_fwd, 0, zh, 0), (y_fwd, 0, zh, 1), (z_step, 1, 1), (z_step, 2, 0), (z_step, 2, 1),
            (x_end, 0), (g_got,), (gf_task, 0), (zh_got, 0), (z_step, 3, 0, 0), (z_step, 3, 1, 0), (x_fwd, 1), (x_out, 3, 0), (x_out, 3, 1), (zh_send, 1),
            (y_end, 0, zh, 0), (gs_task, zh, 0), (y_fwd, 1, 1 - zh, 0), (x_fwd, 2), (y_end, 0, zh, 1), (gs_task, zh, 1),
            (x_end, 1), (gf_task, 1), (own, first, ya, 0, 1 - zh), (relay, first, yb, 0, 1 - zh),
            (zh_got, 1), (x_fwd, 3), (y_end, 1, 1 - zh, 0), (gs_task, 1 - zh, 0), (xa, 0), (xb, 0), (xa, 3), (xb, 3),
            (relay, first, yc, 0, 1 - zh), (y_fwd, 1, 1 - zh, 1), (x_end, 2), (gf_task, 2), (xc, 0), (own, first, tz),
            (y_end, 1, 1 - zh, 1), (gs_task, 1 - zh, 1), (xa, 2), (xb, 2), (xa, 1),
            (x_end, 3), (gf_task, 3), (own, 1 - first, ya, 0, 1 - zh), (relay, 1 - first, yb, 0, 1 - zh), (own, first, ya, 1, zh), (relay, first, yb, 1, zh),
            (relay, 1 - first, yc, 0, 1 - zh), (xc, 2), (xb, 1), (x_got, 0), (z_mid, 0, 0), (relay, first, yc, 1, zh), (own, 1 - first, ya, 1, zh), (relay, 1 - first, yb, 1, zh),
            (own, 1 - first, tz), (z_mid, 0, 1), (xc, 1), (xc, 3),
            (x_got, 2), (z_mid, 2, 0), (relay, 1 - first, yc, 1, zh), (z_mid, 2, 1), (x_got, 1), (z_mid, 1, 0), (z_mid, 1, 1),
            (gf_end,), (gf_out,),
            (x_got, 3), (gs_out, 0), (gs_out, 1),
        )
        finish(1)


def local(embed_first, embed_second, corr_grad):
    dma = pltpu.SemaphoreType.DMA
    vm = pltpu.VMEM
    hbm = lambda a: pltpu.with_memory_space_constraint(a, pltpu.HBM)
    gf, gs = pl.pallas_call(
        kernel,
        out_shape=(jax.ShapeDtypeStruct((2, 2, 48, 512), BF), jax.ShapeDtypeStruct((48, 2048), BF)),
        in_specs=[pl.BlockSpec(memory_space=pl.ANY)] * 3,
        out_specs=[pl.BlockSpec(memory_space=pltpu.VMEM)] * 2,
        scratch_shapes=[
            vm((2, 2, 48, 512), BF),
            vm((8, 2, 2, 48, 512), BF),
            vm((4, 4, 2, 48, 1024), BF),
            vm((4, 128, 2048), F32),
            vm((2, 512, 2048), BF),
            vm((4, 4, 2, 48, 1024), BF),
            vm((8, 2, 2, 48, 512), BF),
            vm((4, 2, 48, 1024), BF),
            vm((4, 2, 2, 48, 1024), BF),
            vm((2, 2, 2, 48, 512), BF),
            vm((2, 2, 2, 2, 48, 512), BF),
            vm((3, 2, 48, 1024), BF),
            vm((2, 2, 48, 1024), BF),
            vm((3, 2, 48, 1024), BF),
            vm((2, 2, 48, 512), BF),
            vm((2, 2, 48, 512), BF),
            vm((2, 2, 48, 512), BF),
            vm((2, 48, 512), BF),
            dma((4,)), dma((4,)),
            dma((6,)), dma((6,)),
            dma((2, 2)), dma((2, 2)),
            dma((5, 2)), dma((4, 2)),
            dma((2, 3, 2)), dma((2, 3, 2)),
            dma((4, 3, 2)), dma((4, 3, 2)),
            dma((4, 3, 2)), dma((4, 3, 2)),
            dma((2, 3, 2)), dma((2, 3, 2)),
            dma((3, 2)), dma((5, 2)),
        ],
        compiler_params=pltpu.CompilerParams(
            collective_id=0, has_side_effects=True, vmem_limit_bytes=50 * 2**20
        ),
    )(hbm(embed_first.reshape(2, 2, 48, 512)), hbm(embed_second), hbm(corr_grad))
    return gf.reshape(192, 512), gs


def solution(mesh):
    return jax.shard_map(
        local,
        mesh=mesh,
        in_specs=(P("col", "row"), P("row", "col"), P("row", "col")),
        out_specs=(P("col", "row"), P("row", "col")),
        check_vma=False,
    )
```

```python
import jax
import jax.numpy as jnp
from jax import lax
from jax.experimental import pallas as pl
from jax.experimental.pallas import tpu as pltpu
from jax.sharding import PartitionSpec as P

BF = jnp.bfloat16
F32 = jnp.float32
MESH = pl.DeviceIdType.MESH


def kernel(e1_hbm, e2_hbm, g_hbm, gf_ref, gs_ref,
           e1s, E1, E2, gst, G, PS, PF, XA, XB, YA, YB, ZO, ZI, SZ, TZ, ZH, FS, FX,
           lsem, gsem, cs, cr, es, er, zs, zr, ys, yr, xs, xr, ps, pr, fs, fr, ss, sr):
    row = lax.axis_index("row")
    col = lax.axis_index("col")
    x, p, c = row // 8, (row // 2) % 4, row % 2
    zh, y = col // 4, col % 4
    s = 1 - 2 * (p // 2)
    mid = ((p + 1) // 2) % 2
    first = p // 2

    def dev(x_=x, p_=p, c_=c, zh_=zh, y_=y):
        return ((x_ * 4 + p_) * 2 + c_, zh_ * 4 + y_)

    xp, xm, xo = (x + 1) % 4, (x + 3) % 4, (x + 2) % 4
    yp, ym, yo = (y + 1) % 4, (y + 3) % 4, (y + 2) % 4
    d_core = dev(c_=1 - c)
    d_xp, d_xm = dev(x_=xp), dev(x_=xm)
    d_yp, d_ym = dev(y_=yp), dev(y_=ym)
    d_zh = dev(zh_=1 - zh)
    d_in = dev(p_=p + s)
    d_out = dev(p_=(p - s + 4) % 4)

    sends, side = [], [0]

    def rc(src, dst, ssem, rsem, d):
        return pltpu.make_async_remote_copy(src, dst, ssem, rsem, device_id=d, device_id_type=MESH)

    def go(src, dst, sems, i, rsem, d):
        go_if(None, src, dst, sems, i, rsem, d)

    def go_if(when, src, dst, sems, i, rsem, d):
        rc(src, dst, sems.at[i], rsem, d).start()
        if not any(w == when and a is sems and b == i for w, a, b in sends):
            sends.append((when, sems, i))

    def got(dst, rsem):
        rc(dst, dst, rsem, rsem, d_core).wait_recv()

    o = [p + s * (mid * m + (1 - mid) * e) for m, e in ((0, 0), (-1, 1), (1, 2), (2, 3))]
    t = [p + s * (mid * m + (1 - mid) * e) for m, e in ((2, 3), (1, 2), (-1, 1), (0, 0))]

    l2 = [pltpu.make_async_copy(e2_hbm.at[:, pl.ds(h * 1024, 1024)], E2.at[p, x, h], lsem.at[h]) for h in range(2)]
    l1 = pltpu.make_async_copy(e1_hbm, e1s, lsem.at[2])
    l1own = pltpu.make_async_copy(e1_hbm.at[:, c], E1.at[col, :, c], lsem.at[3])
    for cp in l2:
        cp.start()
    l1.start()
    l1own.start()
    lg = [pltpu.make_async_copy(g_hbm.at[pl.ds(i * 128, 128)], gst.at[i], gsem.at[i]) for i in range(4)]

    barrier = pltpu.get_barrier_semaphore()
    for d in (d_core, d_xp, d_xm, d_yp, d_ym, d_zh, d_in):
        pl.semaphore_signal(barrier, 1, device_id=d, device_id_type=MESH)

    @pl.when(mid == 1)
    def _():
        pl.semaphore_signal(barrier, 1, device_id=d_out, device_id_type=MESH)

    pl.semaphore_wait(barrier, 7 + mid)

    for cp in l2:
        cp.wait()

    @pl.when(mid == 1)
    def _():
        for h in range(2):
            go_if(1, E2.at[p, x, h], E2.at[p, x, h], zs, (0, h), zr.at[0, h], d_in)
            go_if(1, E2.at[p, x, h], E2.at[p, x, h], zs, (1, h), zr.at[0, h], d_out)

    @pl.when(mid == 0)
    def _():
        for h in range(2):
            go_if(0, E2.at[p, x, h], E2.at[p, x, h], zs, (0, h), zr.at[3, h], d_in)

    def x_send(k, r, h):
        go(E2.at[o[k], x, h], E2.at[o[k], x, h], xs, (k, r, h,), xr.at[k, r, h], (d_xp, d_xm)[r])

    def x_fwd(k):
        for r, frm, to in ((0, xm, d_xp), (1, xp, d_xm)):
            got(E2.at[o[k], frm, r], xr.at[k, r, r])
            go(E2.at[o[k], frm, r], E2.at[o[k], frm, r], xs, (k, 2, r,), xr.at[k, 2, r], to)

    def x_end(k):
        got(E2.at[o[k], xm, 1], xr.at[k, 0, 1])
        got(E2.at[o[k], xp, 0], xr.at[k, 1, 0])
        got(E2.at[o[k], xo, 0], xr.at[k, 2, 0])
        got(E2.at[o[k], xo, 1], xr.at[k, 2, 1])

    zslot = [None] + [mid * m + (1 - mid) * e for m, e in ((3, 0), (0, 1), (1, 2))]

    def x_out(k, h):
        x_send(k, 0, h)
        x_send(k, 1, h)

    def z_step(k, h, out=1):
        got(E2.at[o[k], x, h], zr.at[zslot[k], h])
        if out:
            x_out(k, h)

        if side[0]:
            d = d_in if k == 1 else d_out
            slot = 1 if k < 3 else 2
            go_if(1, E2.at[o[k], x, h], E2.at[o[k], x, h], zs, (k + 1, h), zr.at[slot, h], d)

    for r, h in ((0, 0), (1, 1), (0, 1), (1, 0)):
        x_send(0, r, h)

    l1.wait()
    go(e1s.at[:, 1 - c], E1.at[col, :, c], cs, (0,), cr.at[0], d_core)
    for cp in lg:
        cp.start()
    l1own.wait()
    got(E1.at[col, :, 1 - c], cr.at[0])

    w0 = (p + 1 + mid) % 2
    half = (w0, 1 - w0)

    def y_send(i, q, r, h):
        b = E1.at[q * 4 + y, half[h]]
        go(b, b, ys, (i, r, h), yr.at[i, r, h], (d_yp, d_ym)[r])

    def y_fwd(i, q, r):
        frm, to = ((q * 4 + ym, d_yp), (q * 4 + yp, d_ym))[r]
        got(E1.at[frm, half[r]], yr.at[i, r, r])
        go(E1.at[frm, half[r]], E1.at[frm, half[r]], ys, (i, 2, r), yr.at[i, 2, r], to)

    def y_end(i, q, h):
        got(E1.at[q * 4 + (yp, ym)[h], half[h]], yr.at[i, 1 - h, h])
        got(E1.at[q * 4 + yo, half[h]], yr.at[i, 2, h])

    for r, h in ((0, 0), (1, 1), (0, 1), (1, 0)):
        y_send(0, zh, r, h)

    def zh_send(*hs):
        for h in hs:
            b = E1.at[col, half[h]]
            go(b, b, es, (0, h), er.at[0, h], d_zh)

    def zh_got(h):
        got(E1.at[(1 - zh) * 4 + y, half[h]], er.at[0, h])
        y_send(1, 1 - zh, 0, h)
        y_send(1, 1 - zh, 1, h)

    def g_share():
        for i in range(4):
            lg[i].wait()
            b = G.at[c, pl.ds(i * 128, 128)]
            G[c, pl.ds(i * 128, 128), :] = gst[i].astype(BF)
            go(b, b, cs, (1 + i,), cr.at[1 + i], d_core)

    def g_got():
        for i in range(4):
            got(G.at[1 - c, pl.ds(i * 128, 128)], cr.at[1 + i])

    def gf_task(k):
        ok = o[k]
        a, i = ok // 2, ok % 2

        def body(h, carry):
            acc = None
            for hj in range(2):
                lhs = E2[ok, :, hj].reshape(192, 1024)
                r = lax.dot_general(lhs, G[h, :, pl.ds(hj * 1024, 1024)], (((1,), (1,)), ((), ())),
                                    preferred_element_type=F32)
                acc = r if acc is None else acc + r
            acc = acc.astype(BF).reshape(4, 48, 512)
            for n in range(4):
                PF[2 * n + a, h, i] = acc[n]
            return carry
        lax.fori_loop(0, 2, body, 0)

    def gs_task(q, w):
        def body(n, carry):
            acc = None
            for h in range(2):
                lhs = E1[pl.ds(4 * q, 4), half[w], h].reshape(192, 512)
                r = jnp.dot(lhs, G[h, :, pl.ds(pl.multiple_of(n * 512, 512), 512)], preferred_element_type=F32)
                acc = r if acc is None else acc + r
            acc = acc.astype(BF).reshape(4, 48, 512)
            for j in range(4):
                PS[2 * q + j // 2, 2 * (j % 2) + half[w], n // 2, :, pl.ds(pl.multiple_of((n % 2) * 512, 512), 512)] = acc[j]
            return carry
        lax.fori_loop(0, 4, body, 0)

    def xa(k):
        for r, d in ((0, d_xp), (1, d_xm)):
            go(PS.at[xo, t[k], r], XA.at[k, r], ps, (k, 0, r,), pr.at[k, 0, r], d)

    def xb(k):
        for r, n, d in ((0, xp, d_xp), (1, xm, d_xm)):
            go(PS.at[n, t[k], 1 - r], XB.at[k, r, 1 - r], ps, (k, 1, r,), pr.at[k, 1, r], d)

    def xc(k):
        for r, n, d in ((0, xp, d_xp), (1, xm, d_xm)):
            got(XA.at[k, r], pr.at[k, 0, r])
            PS[n, t[k], r] = (PS[n, t[k], r].astype(F32) + XA[k, r].astype(F32)).astype(BF)
            go(PS.at[n, t[k], r], XB.at[k, r, r], ps, (k, 2, r,), pr.at[k, 2, r], d)

    def x_got(k):
        for r in range(2):
            got(XB.at[k, r, 1 - r], pr.at[k, 1, r])
            got(XB.at[k, r, r], pr.at[k, 2, r])

    def x_sum(k, h):
        return PS[x, t[k], h].astype(F32) + XB[k, 0, h].astype(F32) + XB[k, 1, h].astype(F32)

    def ya(i, q):
        for r, d in ((0, d_yp), (1, d_ym)):
            go(PF.at[q * 4 + yo, r], YA.at[i, r], fs, (i, 0, r,), fr.at[i, 0, r], d)

    def yb(i, q):
        for r, n, d in ((0, yp, d_yp), (1, ym, d_ym)):
            go(PF.at[q * 4 + n, 1 - r], YB.at[i, r, 1 - r], fs, (i, 1, r,), fr.at[i, 1, r], d)

    def yc(i, q):
        for r, n, d in ((0, yp, d_yp), (1, ym, d_ym)):
            got(YA.at[i, r], fr.at[i, 0, r])
            PF[q * 4 + n, r] = (PF[q * 4 + n, r].astype(F32) + YA[i, r].astype(F32)).astype(BF)
            go(PF.at[q * 4 + n, r], YB.at[i, r, r], fs, (i, 2, r,), fr.at[i, 2, r], d)

    def y_sum(i, q):
        for r in range(2):
            got(YB.at[i, r, 1 - r], fr.at[i, 1, r])
            got(YB.at[i, r, r], fr.at[i, 2, r])
        return PF[q * 4 + y].astype(F32) + YB[i, 0].astype(F32) + YB[i, 1].astype(F32)

    def z_end(k):
        for h in range(2):
            SZ[k, h] = x_sum(k, h).astype(BF)
            go_if(0, SZ.at[k, h], ZO.at[2 - k, h], ss, (k, h), sr.at[2 - k, h], d_in)

    def z_mid(k, h):
        buf, slot = ((ZO.at[2], 2), (ZO.at[1], 1), (ZI.at[1], 4))[k]
        got(buf.at[h], sr.at[slot, h])
        SZ[k, h] = (x_sum(k, h) + buf[h].astype(F32)).astype(BF)
        to, d = ((1, d_in), (0, d_in), (0, d_out))[k]
        go_if(1, SZ.at[k, h], ZI.at[to, h], ss, (k, h), sr.at[3 + to, h], d)

    def tz():
        TZ[...] = y_sum(0, 1 - zh).astype(BF)
        for h in range(2):
            go(TZ.at[h], ZH.at[h], es, (1, h,), er.at[1, h], d_zh)

    def own(cl, f, *a):
        @pl.when((y + cl) % 2 == 0)
        def _():
            f(*a)

    def relay(cl, f, *a):
        @pl.when((y + cl) % 2 == 1)
        def _():
            f(*a)

    def gf_end():
        mine = y_sum(1, zh)
        for h in range(2):
            got(ZH.at[h], er.at[1, h])
        FS[...] = (mine + ZH[...].astype(F32)).astype(BF)
        go(FS.at[1 - c], FX, cs, (5,), cr.at[5], d_core)
        gf_ref[:, c] = FS[c]

    def gf_out():
        got(FX, cr.at[5])
        gf_ref[:, 1 - c] = FX[...]

    def gs_out(h):
        got(ZI.at[0, h], sr.at[3, h])

        total = x_sum(3, h) + ZI[0, h].astype(F32)
        if side[0]:
            got(ZO.at[0, h], sr.at[0, h])
            total = total + ZO[0, h].astype(F32)
        gs_ref[:, pl.ds(h * 1024, 1024)] = total.astype(BF)

    def run(*steps):
        for f, *a in steps:
            with jax.named_scope(f.__name__ + "_".join(getattr(v, "__name__", str(v)) if isinstance(v, int) or callable(v) else "v" for v in a)):
                f(*a)

    def finish(w):
        for when, sems, i in sends:
            if when is None or when == w:
                like = G.at[0, pl.ds(0, 128)] if sems is cs and 1 <= i[0] <= 4 else SZ.at[0, 0]
                rc(like, like, sems.at[i], sr.at[0, 0], d_core).wait_send()

    @pl.when(mid == 0)
    def _():
        side[0] = 0
        run(
            (zh_send, 0), (g_share,), (x_fwd, 0), (z_step, 1, 0), (y_fwd, 0, zh, 0), (y_fwd, 0, zh, 1), (z_step, 1, 1), (zh_got, 0),
            (x_end, 0), (g_got,), (gf_task, 0), (x_fwd, 1), (z_step, 2, 0), (y_end, 0, zh, 0), (gs_task, zh, 0), (z_step, 2, 1), (zh_send, 1),
            (y_fwd, 1, 1 - zh, 0), (z_step, 3, 0), (x_end, 1), (gf_task, 1), (own, first, ya, 0, 1 - zh), (relay, first, yb, 0, 1 - zh),
            (z_step, 3, 1), (zh_got, 1), (x_fwd, 2), (y_end, 1, 1 - zh, 0), (gs_task, 1 - zh, 0), (xa, 0),
            (relay, first, yc, 0, 1 - zh), (y_end, 0, zh, 1), (gs_task, zh, 1), (x_fwd, 3), (xb, 0), (y_fwd, 1, 1 - zh, 1),
            (own, first, tz), (x_end, 2), (gf_task, 2), (xc, 0),
            (y_end, 1, 1 - zh, 1), (gs_task, 1 - zh, 1), (xa, 1), (xb, 1), (xa, 2), (x_end, 3), (gf_task, 3),
            (own, 1 - first, ya, 0, 1 - zh), (relay, 1 - first, yb, 0, 1 - zh), (own, first, ya, 1, zh), (relay, first, yb, 1, zh),
            (x_got, 0), (z_end, 0), (relay, 1 - first, yc, 0, 1 - zh), (xc, 1), (xb, 2), (relay, first, yc, 1, zh),
            (own, 1 - first, ya, 1, zh), (relay, 1 - first, yb, 1, zh), (own, 1 - first, tz), (xc, 2), (xa, 3), (xb, 3),
            (x_got, 1), (z_end, 1), (relay, 1 - first, yc, 1, zh), (x_got, 2), (z_end, 2), (xc, 3),
            (gf_end,), (gf_out,),
            (x_got, 3), (gs_out, 0), (gs_out, 1),
        )
        finish(0)

    @pl.when(mid == 1)
    def _():
        side[0] = 1
        run(
            (zh_send, 0), (g_share,), (x_fwd, 0), (z_step, 1, 0), (y_fwd, 0, zh, 0), (y_fwd, 0, zh, 1), (z_step, 1, 1), (z_step, 2, 0), (z_step, 2, 1),
            (x_end, 0), (g_got,), (gf_task, 0), (zh_got, 0), (z_step, 3, 0, 0), (z_step, 3, 1, 0), (x_fwd, 1), (x_out, 3, 0), (x_out, 3, 1), (zh_send, 1),
            (y_end, 0, zh, 0), (gs_task, zh, 0), (y_fwd, 1, 1 - zh, 0), (x_fwd, 2), (y_end, 0, zh, 1), (gs_task, zh, 1),
            (x_end, 1), (gf_task, 1), (own, first, ya, 0, 1 - zh), (relay, first, yb, 0, 1 - zh),
            (zh_got, 1), (x_fwd, 3), (y_end, 1, 1 - zh, 0), (gs_task, 1 - zh, 0), (xa, 0), (xb, 0), (xa, 3), (xb, 3),
            (relay, first, yc, 0, 1 - zh), (y_fwd, 1, 1 - zh, 1), (x_end, 2), (gf_task, 2), (own, first, tz), (x_end, 3), (gf_task, 3),
            (own, 1 - first, ya, 0, 1 - zh), (relay, 1 - first, yb, 0, 1 - zh), (xc, 0),
            (y_end, 1, 1 - zh, 1), (gs_task, 1 - zh, 1), (xa, 2), (xb, 2), (xa, 1), (own, first, ya, 1, zh), (relay, first, yb, 1, zh),
            (relay, 1 - first, yc, 0, 1 - zh), (relay, first, yc, 1, zh), (own, 1 - first, ya, 1, zh), (relay, 1 - first, yb, 1, zh),
            (x_got, 0), (own, 1 - first, tz), (z_mid, 0, 0), (xc, 2), (xb, 1), (z_mid, 0, 1), (xc, 1), (xc, 3),
            (x_got, 2), (z_mid, 2, 0), (relay, 1 - first, yc, 1, zh), (z_mid, 2, 1), (x_got, 1), (z_mid, 1, 0), (z_mid, 1, 1),
            (gf_end,), (gf_out,),
            (x_got, 3), (gs_out, 0), (gs_out, 1),
        )
        finish(1)


def local(embed_first, embed_second, corr_grad):
    dma = pltpu.SemaphoreType.DMA
    vm = pltpu.VMEM
    hbm = lambda a: pltpu.with_memory_space_constraint(a, pltpu.HBM)
    gf, gs = pl.pallas_call(
        kernel,
        out_shape=(jax.ShapeDtypeStruct((2, 2, 48, 512), BF), jax.ShapeDtypeStruct((48, 2048), BF)),
        in_specs=[pl.BlockSpec(memory_space=pl.ANY)] * 3,
        out_specs=[pl.BlockSpec(memory_space=pltpu.VMEM)] * 2,
        scratch_shapes=[
            vm((2, 2, 48, 512), BF),
            vm((8, 2, 2, 48, 512), BF),
            vm((4, 4, 2, 48, 1024), BF),
            vm((4, 128, 2048), F32),
            vm((2, 512, 2048), BF),
            vm((4, 4, 2, 48, 1024), BF),
            vm((8, 2, 2, 48, 512), BF),
            vm((4, 2, 48, 1024), BF),
            vm((4, 2, 2, 48, 1024), BF),
            vm((2, 2, 2, 48, 512), BF),
            vm((2, 2, 2, 2, 48, 512), BF),
            vm((3, 2, 48, 1024), BF),
            vm((2, 2, 48, 1024), BF),
            vm((3, 2, 48, 1024), BF),
            vm((2, 2, 48, 512), BF),
            vm((2, 2, 48, 512), BF),
            vm((2, 2, 48, 512), BF),
            vm((2, 48, 512), BF),
            dma((4,)), dma((4,)),
            dma((6,)), dma((6,)),
            dma((2, 2)), dma((2, 2)),
            dma((5, 2)), dma((4, 2)),
            dma((2, 3, 2)), dma((2, 3, 2)),
            dma((4, 3, 2)), dma((4, 3, 2)),
            dma((4, 3, 2)), dma((4, 3, 2)),
            dma((2, 3, 2)), dma((2, 3, 2)),
            dma((3, 2)), dma((5, 2)),
        ],
        compiler_params=pltpu.CompilerParams(
            collective_id=0, has_side_effects=True, vmem_limit_bytes=50 * 2**20
        ),
    )(hbm(embed_first.reshape(2, 2, 48, 512)), hbm(embed_second), hbm(corr_grad))
    return gf.reshape(192, 512), gs


def solution(mesh):
    return jax.shard_map(
        local,
        mesh=mesh,
        in_specs=(P("col", "row"), P("row", "col"), P("row", "col")),
        out_specs=(P("col", "row"), P("row", "col")),
        check_vma=False,
    )
```

```python
import jax
import jax.numpy as jnp
from jax import lax
from jax.experimental import pallas as pl
from jax.experimental.pallas import tpu as pltpu
from jax.sharding import PartitionSpec as P

BF = jnp.bfloat16
F32 = jnp.float32
MESH = pl.DeviceIdType.MESH


def kernel(e1_hbm, e2_hbm, g_hbm, gf_ref, gs_ref,
           e1s, E1, E2, gst, G, PS, PF, XA, XB, YA, YB, ZO, ZI, SZ, TZ, ZH, FS, FX,
           lsem, gsem, cs, cr, es, er, zs, zr, ys, yr, xs, xr, ps, pr, fs, fr, ss, sr):
    row = lax.axis_index("row")
    col = lax.axis_index("col")
    x, p, c = row // 8, (row // 2) % 4, row % 2
    zh, y = col // 4, col % 4
    s = 1 - 2 * (p // 2)
    mid = ((p + 1) // 2) % 2
    first = p // 2

    def dev(x_=x, p_=p, c_=c, zh_=zh, y_=y):
        return ((x_ * 4 + p_) * 2 + c_, zh_ * 4 + y_)

    xp, xm, xo = (x + 1) % 4, (x + 3) % 4, (x + 2) % 4
    yp, ym, yo = (y + 1) % 4, (y + 3) % 4, (y + 2) % 4
    d_core = dev(c_=1 - c)
    d_xp, d_xm = dev(x_=xp), dev(x_=xm)
    d_yp, d_ym = dev(y_=yp), dev(y_=ym)
    d_zh = dev(zh_=1 - zh)
    d_in = dev(p_=p + s)
    d_out = dev(p_=(p - s + 4) % 4)

    sends, side = [], [0]

    def rc(src, dst, ssem, rsem, d):
        return pltpu.make_async_remote_copy(src, dst, ssem, rsem, device_id=d, device_id_type=MESH)

    def go(src, dst, sems, i, rsem, d):
        go_if(None, src, dst, sems, i, rsem, d)

    def go_if(when, src, dst, sems, i, rsem, d):
        rc(src, dst, sems.at[i], rsem, d).start()
        if not any(w == when and a is sems and b == i for w, a, b in sends):
            sends.append((when, sems, i))

    def got(dst, rsem):
        rc(dst, dst, rsem, rsem, d_core).wait_recv()

    o = [p + s * (mid * m + (1 - mid) * e) for m, e in ((0, 0), (-1, 1), (1, 2), (2, 3))]
    t = [p + s * (mid * m + (1 - mid) * e) for m, e in ((2, 3), (1, 2), (-1, 1), (0, 0))]

    l2 = [pltpu.make_async_copy(e2_hbm.at[:, pl.ds(h * 1024, 1024)], E2.at[p, x, h], lsem.at[h]) for h in range(2)]
    l1 = pltpu.make_async_copy(e1_hbm, e1s, lsem.at[2])
    l1own = pltpu.make_async_copy(e1_hbm.at[:, c], E1.at[col, :, c], lsem.at[3])
    for cp in l2:
        cp.start()
    l1.start()
    l1own.start()
    lg = [pltpu.make_async_copy(g_hbm.at[pl.ds(i * 128, 128)], gst.at[i], gsem.at[i]) for i in range(4)]

    barrier = pltpu.get_barrier_semaphore()
    for d in (d_core, d_xp, d_xm, d_yp, d_ym, d_zh, d_in):
        pl.semaphore_signal(barrier, 1, device_id=d, device_id_type=MESH)

    @pl.when(mid == 1)
    def _():
        pl.semaphore_signal(barrier, 1, device_id=d_out, device_id_type=MESH)

    pl.semaphore_wait(barrier, 7 + mid)

    for cp in l2:
        cp.wait()

    @pl.when(mid == 1)
    def _():
        for h in range(2):
            go_if(1, E2.at[p, x, h], E2.at[p, x, h], zs, (0, h), zr.at[0, h], d_in)
            go_if(1, E2.at[p, x, h], E2.at[p, x, h], zs, (1, h), zr.at[0, h], d_out)

    @pl.when(mid == 0)
    def _():
        for h in range(2):
            go_if(0, E2.at[p, x, h], E2.at[p, x, h], zs, (0, h), zr.at[3, h], d_in)

    def x_send(k, r, h):
        go(E2.at[o[k], x, h], E2.at[o[k], x, h], xs, (k, r, h,), xr.at[k, r, h], (d_xp, d_xm)[r])

    def x_fwd(k):
        for r, frm, to in ((0, xm, d_xp), (1, xp, d_xm)):
            got(E2.at[o[k], frm, r], xr.at[k, r, r])
            go(E2.at[o[k], frm, r], E2.at[o[k], frm, r], xs, (k, 2, r,), xr.at[k, 2, r], to)

    def x_end(k):
        got(E2.at[o[k], xm, 1], xr.at[k, 0, 1])
        got(E2.at[o[k], xp, 0], xr.at[k, 1, 0])
        got(E2.at[o[k], xo, 0], xr.at[k, 2, 0])
        got(E2.at[o[k], xo, 1], xr.at[k, 2, 1])

    zslot = [None] + [mid * m + (1 - mid) * e for m, e in ((3, 0), (0, 1), (1, 2))]

    def x_out(k, h):
        x_send(k, 0, h)
        x_send(k, 1, h)

    def z_step(k, h, out=1):
        got(E2.at[o[k], x, h], zr.at[zslot[k], h])
        if out:
            x_out(k, h)

        if side[0]:
            d = d_in if k == 1 else d_out
            slot = 1 if k < 3 else 2
            go_if(1, E2.at[o[k], x, h], E2.at[o[k], x, h], zs, (k + 1, h), zr.at[slot, h], d)

    for r, h in ((0, 0), (1, 1), (0, 1), (1, 0)):
        x_send(0, r, h)

    l1.wait()
    go(e1s.at[:, 1 - c], E1.at[col, :, c], cs, (0,), cr.at[0], d_core)
    for cp in lg:
        cp.start()
    l1own.wait()
    got(E1.at[col, :, 1 - c], cr.at[0])

    w0 = (p + 1 + mid) % 2
    half = (w0, 1 - w0)

    def y_send(i, q, r, h):
        b = E1.at[q * 4 + y, half[h]]
        go(b, b, ys, (i, r, h), yr.at[i, r, h], (d_yp, d_ym)[r])

    def y_fwd(i, q, r):
        frm, to = ((q * 4 + ym, d_yp), (q * 4 + yp, d_ym))[r]
        got(E1.at[frm, half[r]], yr.at[i, r, r])
        go(E1.at[frm, half[r]], E1.at[frm, half[r]], ys, (i, 2, r), yr.at[i, 2, r], to)

    def y_end(i, q, h):
        got(E1.at[q * 4 + (yp, ym)[h], half[h]], yr.at[i, 1 - h, h])
        got(E1.at[q * 4 + yo, half[h]], yr.at[i, 2, h])

    for r in range(2):
        y_send(0, zh, r, 0)

    def y_rest():
        for r in range(2):
            y_send(0, zh, r, 1)

    def zh_send(*hs):
        for h in hs:
            b = E1.at[col, half[h]]
            go(b, b, es, (0, h), er.at[0, h], d_zh)

    def zh_got(h):
        got(E1.at[(1 - zh) * 4 + y, half[h]], er.at[0, h])
        y_send(1, 1 - zh, 0, h)
        y_send(1, 1 - zh, 1, h)

    def g_share():
        for i in range(4):
            lg[i].wait()
            b = G.at[c, pl.ds(i * 128, 128)]
            G[c, pl.ds(i * 128, 128), :] = gst[i].astype(BF)
            go(b, b, cs, (1 + i,), cr.at[1 + i], d_core)

    def g_got():
        for i in range(4):
            got(G.at[1 - c, pl.ds(i * 128, 128)], cr.at[1 + i])

    def gf_task(k):
        ok = o[k]
        a, i = ok // 2, ok % 2

        def body(h, carry):
            acc = None
            for hj in range(2):
                lhs = E2[ok, :, hj].reshape(192, 1024)
                r = lax.dot_general(lhs, G[h, :, pl.ds(hj * 1024, 1024)], (((1,), (1,)), ((), ())),
                                    preferred_element_type=F32)
                acc = r if acc is None else acc + r
            acc = acc.astype(BF).reshape(4, 48, 512)
            for n in range(4):
                PF[2 * n + a, h, i] = acc[n]
            return carry
        lax.fori_loop(0, 2, body, 0)

    def gs_task(q, w):
        def body(n, carry):
            acc = None
            for h in range(2):
                lhs = E1[pl.ds(4 * q, 4), half[w], h].reshape(192, 512)
                r = jnp.dot(lhs, G[h, :, pl.ds(pl.multiple_of(n * 512, 512), 512)], preferred_element_type=F32)
                acc = r if acc is None else acc + r
            acc = acc.astype(BF).reshape(4, 48, 512)
            for j in range(4):
                PS[2 * q + j // 2, 2 * (j % 2) + half[w], n // 2, :, pl.ds(pl.multiple_of((n % 2) * 512, 512), 512)] = acc[j]
            return carry
        lax.fori_loop(0, 4, body, 0)

    def xa(k):
        for r, d in ((0, d_xp), (1, d_xm)):
            go(PS.at[xo, t[k], r], XA.at[k, r], ps, (k, 0, r,), pr.at[k, 0, r], d)

    def xb(k):
        for r, n, d in ((0, xp, d_xp), (1, xm, d_xm)):
            go(PS.at[n, t[k], 1 - r], XB.at[k, r, 1 - r], ps, (k, 1, r,), pr.at[k, 1, r], d)

    def xc(k):
        for r, n, d in ((0, xp, d_xp), (1, xm, d_xm)):
            got(XA.at[k, r], pr.at[k, 0, r])
            PS[n, t[k], r] = (PS[n, t[k], r].astype(F32) + XA[k, r].astype(F32)).astype(BF)
            go(PS.at[n, t[k], r], XB.at[k, r, r], ps, (k, 2, r,), pr.at[k, 2, r], d)

    def x_got(k):
        for r in range(2):
            got(XB.at[k, r, 1 - r], pr.at[k, 1, r])
            got(XB.at[k, r, r], pr.at[k, 2, r])

    def x_sum(k, h):
        return PS[x, t[k], h].astype(F32) + XB[k, 0, h].astype(F32) + XB[k, 1, h].astype(F32)

    def ya(i, q):
        for r, d in ((0, d_yp), (1, d_ym)):
            go(PF.at[q * 4 + yo, r], YA.at[i, r], fs, (i, 0, r,), fr.at[i, 0, r], d)

    def yb(i, q):
        for r, n, d in ((0, yp, d_yp), (1, ym, d_ym)):
            go(PF.at[q * 4 + n, 1 - r], YB.at[i, r, 1 - r], fs, (i, 1, r,), fr.at[i, 1, r], d)

    def yc(i, q):
        for r, n, d in ((0, yp, d_yp), (1, ym, d_ym)):
            got(YA.at[i, r], fr.at[i, 0, r])
            PF[q * 4 + n, r] = (PF[q * 4 + n, r].astype(F32) + YA[i, r].astype(F32)).astype(BF)
            go(PF.at[q * 4 + n, r], YB.at[i, r, r], fs, (i, 2, r,), fr.at[i, 2, r], d)

    def y_sum(i, q):
        for r in range(2):
            got(YB.at[i, r, 1 - r], fr.at[i, 1, r])
            got(YB.at[i, r, r], fr.at[i, 2, r])
        return PF[q * 4 + y].astype(F32) + YB[i, 0].astype(F32) + YB[i, 1].astype(F32)

    def z_end(k):
        for h in range(2):
            SZ[k, h] = x_sum(k, h).astype(BF)
            go_if(0, SZ.at[k, h], ZO.at[2 - k, h], ss, (k, h), sr.at[2 - k, h], d_in)

    def z_mid(k, h):
        buf, slot = ((ZO.at[2], 2), (ZO.at[1], 1), (ZI.at[1], 4))[k]
        got(buf.at[h], sr.at[slot, h])
        SZ[k, h] = (x_sum(k, h) + buf[h].astype(F32)).astype(BF)
        to, d = ((1, d_in), (0, d_in), (0, d_out))[k]
        go_if(1, SZ.at[k, h], ZI.at[to, h], ss, (k, h), sr.at[3 + to, h], d)

    def tz():
        TZ[...] = y_sum(0, 1 - zh).astype(BF)
        for h in range(2):
            go(TZ.at[h], ZH.at[h], es, (1, h,), er.at[1, h], d_zh)

    def own(cl, f, *a):
        @pl.when((y + cl) % 2 == 0)
        def _():
            f(*a)

    def relay(cl, f, *a):
        @pl.when((y + cl) % 2 == 1)
        def _():
            f(*a)

    def gf_end():
        mine = y_sum(1, zh)
        for h in range(2):
            got(ZH.at[h], er.at[1, h])
        FS[...] = (mine + ZH[...].astype(F32)).astype(BF)
        go(FS.at[1 - c], FX, cs, (5,), cr.at[5], d_core)
        gf_ref[:, c] = FS[c]

    def gf_out():
        got(FX, cr.at[5])
        gf_ref[:, 1 - c] = FX[...]

    def gs_out(h):
        got(ZI.at[0, h], sr.at[3, h])

        total = x_sum(3, h) + ZI[0, h].astype(F32)
        if side[0]:
            got(ZO.at[0, h], sr.at[0, h])
            total = total + ZO[0, h].astype(F32)
        gs_ref[:, pl.ds(h * 1024, 1024)] = total.astype(BF)

    def run(*steps):
        for f, *a in steps:
            with jax.named_scope(f.__name__ + "_".join(getattr(v, "__name__", str(v)) if isinstance(v, int) or callable(v) else "v" for v in a)):
                f(*a)

    def finish(w):
        for when, sems, i in sends:
            if when is None or when == w:
                like = G.at[0, pl.ds(0, 128)] if sems is cs and 1 <= i[0] <= 4 else SZ.at[0, 0]
                rc(like, like, sems.at[i], sr.at[0, 0], d_core).wait_send()

    @pl.when(mid == 0)
    def _():
        side[0] = 0
        run(
            (zh_send, 0), (g_share,), (x_fwd, 0), (z_step, 1, 0), (y_rest,), (y_fwd, 0, zh, 0), (z_step, 1, 1), (zh_got, 0),
            (x_end, 0), (g_got,), (gf_task, 0), (x_fwd, 1), (z_step, 2, 0), (y_fwd, 0, zh, 1), (y_end, 0, zh, 0), (gs_task, zh, 0), (z_step, 2, 1), (zh_send, 1),
            (y_fwd, 1, 1 - zh, 0), (z_step, 3, 0), (x_end, 1), (gf_task, 1), (own, first, ya, 0, 1 - zh), (relay, first, yb, 0, 1 - zh),
            (z_step, 3, 1), (zh_got, 1), (x_fwd, 2), (y_end, 1, 1 - zh, 0), (gs_task, 1 - zh, 0), (xa, 0),
            (relay, first, yc, 0, 1 - zh), (y_end, 0, zh, 1), (gs_task, zh, 1), (x_fwd, 3), (xb, 0), (y_fwd, 1, 1 - zh, 1),
            (own, first, tz), (x_end, 2), (gf_task, 2), (xc, 0),
            (y_end, 1, 1 - zh, 1), (gs_task, 1 - zh, 1), (xa, 1), (xb, 1), (xa, 2), (x_end, 3), (gf_task, 3),
            (own, 1 - first, ya, 0, 1 - zh), (relay, 1 - first, yb, 0, 1 - zh), (own, first, ya, 1, zh), (relay, first, yb, 1, zh),
            (x_got, 0), (z_end, 0), (relay, 1 - first, yc, 0, 1 - zh), (xc, 1), (xb, 2), (relay, first, yc, 1, zh),
            (own, 1 - first, ya, 1, zh), (relay, 1 - first, yb, 1, zh), (own, 1 - first, tz), (xc, 2), (xa, 3), (xb, 3),
            (x_got, 1), (z_end, 1), (relay, 1 - first, yc, 1, zh), (x_got, 2), (z_end, 2), (xc, 3),
            (gf_end,), (gf_out,),
            (x_got, 3), (gs_out, 0), (gs_out, 1),
        )
        finish(0)

    @pl.when(mid == 1)
    def _():
        side[0] = 1
        run(
            (zh_send, 0), (g_share,), (x_fwd, 0), (z_step, 1, 0), (y_rest,), (y_fwd, 0, zh, 0), (z_step, 1, 1), (z_step, 2, 0), (z_step, 2, 1),
            (x_end, 0), (g_got,), (gf_task, 0), (y_fwd, 0, zh, 1), (zh_got, 0), (z_step, 3, 0, 0), (z_step, 3, 1, 0), (x_fwd, 1), (x_out, 3, 0), (x_out, 3, 1), (zh_send, 1),
            (y_end, 0, zh, 0), (gs_task, zh, 0), (y_fwd, 1, 1 - zh, 0), (x_fwd, 2), (y_end, 0, zh, 1), (gs_task, zh, 1),
            (x_end, 1), (gf_task, 1), (own, first, ya, 0, 1 - zh), (relay, first, yb, 0, 1 - zh),
            (zh_got, 1), (x_fwd, 3), (y_end, 1, 1 - zh, 0), (gs_task, 1 - zh, 0), (xa, 0), (xb, 0), (xa, 3),
            (relay, first, yc, 0, 1 - zh), (y_fwd, 1, 1 - zh, 1), (x_end, 2), (gf_task, 2), (own, first, tz), (x_end, 3), (gf_task, 3),
            (own, 1 - first, ya, 0, 1 - zh), (relay, 1 - first, yb, 0, 1 - zh), (xc, 0),
            (y_end, 1, 1 - zh, 1), (gs_task, 1 - zh, 1), (xa, 2), (xb, 2), (xa, 1), (own, first, ya, 1, zh), (relay, first, yb, 1, zh),
            (relay, 1 - first, yc, 0, 1 - zh), (relay, first, yc, 1, zh), (own, 1 - first, ya, 1, zh), (relay, 1 - first, yb, 1, zh),
            (x_got, 0), (own, 1 - first, tz), (z_mid, 0, 0), (xc, 2), (xb, 1), (z_mid, 0, 1), (xc, 1), (xb, 3), (xc, 3),
            (x_got, 2), (z_mid, 2, 0), (relay, 1 - first, yc, 1, zh), (z_mid, 2, 1), (x_got, 1), (z_mid, 1, 0), (z_mid, 1, 1),
            (gf_end,), (gf_out,),
            (x_got, 3), (gs_out, 0), (gs_out, 1),
        )
        finish(1)


def local(embed_first, embed_second, corr_grad):
    dma = pltpu.SemaphoreType.DMA
    vm = pltpu.VMEM
    hbm = lambda a: pltpu.with_memory_space_constraint(a, pltpu.HBM)
    gf, gs = pl.pallas_call(
        kernel,
        out_shape=(jax.ShapeDtypeStruct((2, 2, 48, 512), BF), jax.ShapeDtypeStruct((48, 2048), BF)),
        in_specs=[pl.BlockSpec(memory_space=pl.ANY)] * 3,
        out_specs=[pl.BlockSpec(memory_space=pltpu.VMEM)] * 2,
        scratch_shapes=[
            vm((2, 2, 48, 512), BF),
            vm((8, 2, 2, 48, 512), BF),
            vm((4, 4, 2, 48, 1024), BF),
            vm((4, 128, 2048), F32),
            vm((2, 512, 2048), BF),
            vm((4, 4, 2, 48, 1024), BF),
            vm((8, 2, 2, 48, 512), BF),
            vm((4, 2, 48, 1024), BF),
            vm((4, 2, 2, 48, 1024), BF),
            vm((2, 2, 2, 48, 512), BF),
            vm((2, 2, 2, 2, 48, 512), BF),
            vm((3, 2, 48, 1024), BF),
            vm((2, 2, 48, 1024), BF),
            vm((3, 2, 48, 1024), BF),
            vm((2, 2, 48, 512), BF),
            vm((2, 2, 48, 512), BF),
            vm((2, 2, 48, 512), BF),
            vm((2, 48, 512), BF),
            dma((4,)), dma((4,)),
            dma((6,)), dma((6,)),
            dma((2, 2)), dma((2, 2)),
            dma((5, 2)), dma((4, 2)),
            dma((2, 3, 2)), dma((2, 3, 2)),
            dma((4, 3, 2)), dma((4, 3, 2)),
            dma((4, 3, 2)), dma((4, 3, 2)),
            dma((2, 3, 2)), dma((2, 3, 2)),
            dma((3, 2)), dma((5, 2)),
        ],
        compiler_params=pltpu.CompilerParams(
            collective_id=0, has_side_effects=True, vmem_limit_bytes=50 * 2**20
        ),
    )(hbm(embed_first.reshape(2, 2, 48, 512)), hbm(embed_second), hbm(corr_grad))
    return gf.reshape(192, 512), gs


def solution(mesh):
    return jax.shard_map(
        local,
        mesh=mesh,
        in_specs=(P("col", "row"), P("row", "col"), P("row", "col")),
        out_specs=(P("col", "row"), P("row", "col")),
        check_vma=False,
    )
```
